32 devices in a mesh: fsdp: 4 (over z), seq: 4 (over y, x), tp: 2 (over core).
Axes of the slice: x: 2, y: 2, z: 4, core: 2. Of those that a mesh axis runs over, the one named last changes fastest.
Arguments:
- tokens: bfloat16 [4, 8, 256, 384], P(None, 'fsdp', 'seq'), may hold values from -6 to 6
- lengths: int32 [4, 8], P(None, 'fsdp'), may hold values from 64 to 256, as said below
- grad_out: bfloat16 [4, 8, 256, 384], P(None, 'fsdp', 'seq'), may hold values from -6 to 6
- qkv_weight: float32 [3, 384, 384], P(None, 'fsdp', 'tp'), may hold values from -0.3125 to 0.3125
- out_weight: float32 [384, 384], P('tp', 'fsdp'), may hold values from -1.25 to 1.25
- up_weight: float32 [384, 1536], P('fsdp', 'tp'), may hold values from -0.3125 to 0.3125
- down_weight: float32 [1536, 384], P('tp', 'fsdp'), may hold values from -0.15625 to 0.15625
- attn_gain: float32 [384], P('fsdp'), may hold values from 0.25 to 1.75
- ffn_gain: float32 [384], P('fsdp'), may hold values from 0.25 to 1.75
- moment_qkv: float32 [3, 384, 384], P(None, 'fsdp', 'tp'), may hold values from -3 to 3
- moment_out: float32 [384, 384], P('tp', 'fsdp'), may hold values from -3 to 3
- moment_up: float32 [384, 1536], P('fsdp', 'tp'), may hold values from -3 to 3
- moment_down: float32 [1536, 384], P('tp', 'fsdp'), may hold values from -3 to 3
- moment_attn: float32 [384], P('fsdp'), may hold values from -3 to 3
- moment_ffn: float32 [384], P('fsdp'), may hold values from -3 to 3
Outputs:
- block_out: bfloat16 [4, 8, 256, 384], P(None, 'fsdp', 'seq')
- input_grad: float32 [4, 8, 256, 384], P(None, 'fsdp', 'seq')
- qkv_grad: float32 [3, 384, 384], P(None, 'fsdp', 'tp')
- out_grad: float32 [384, 384], P('tp', 'fsdp')
- up_grad: float32 [384, 1536], P('fsdp', 'tp')
- down_grad: float32 [1536, 384], P('tp', 'fsdp')
- attn_gain_grad: float32 [384], P('fsdp')
- ffn_gain_grad: float32 [384], P('fsdp')
- new_qkv: float32 [3, 384, 384], P(None, 'fsdp', 'tp')
- new_out: float32 [384, 384], P('tp', 'fsdp')
- new_up: float32 [384, 1536], P('fsdp', 'tp')
- new_down: float32 [1536, 384], P('tp', 'fsdp')
- new_attn_gain: float32 [384], P('fsdp')
- new_ffn_gain: float32 [384], P('fsdp')
- new_moment_qkv: float32 [3, 384, 384], P(None, 'fsdp', 'tp')
- new_moment_out: float32 [384, 384], P('tp', 'fsdp')
- new_moment_up: float32 [384, 1536], P('fsdp', 'tp')
- new_moment_down: float32 [1536, 384], P('tp', 'fsdp')
- new_moment_attn: float32 [384], P('fsdp')
- new_moment_ffn: float32 [384], P('fsdp')
The draws below stay inside these ranges and needn't reach their ends.
Inputs may be any that keep to these rules, and one draw needn't show every extreme that they name: `lengths`: slots at or past an image's length are padding; in every micro-batch one image has all 256 slots valid and one has 64.
All inputs are finite; a program needn't handle non-finite values.
Results may differ from the reference program's by a relative error of at most 0.012.
The reference program's roundings to bfloat16 on the way count: a program that leaves them out, or rounds other values in their place, can miss the bound.
Values may be sent and summed in bfloat16 or wider, within the bound.
A program may use at most 128 MiB of HBM per device.

```python
import math
import jax
import jax.numpy as jnp
from jax import lax

D = 384
HEADS = 6
HEAD_DIM = 64
FF = 1536
SEQ_LEN = 256
MICRO = 4
NS_STEPS = 5
IMG_DEV = 2
IMAGES = 8
N_FSDP = 4


def draw_lengths(key, part):
    drawn = jax.random.randint(key, (MICRO, IMAGES), SEQ_LEN // 4, SEQ_LEN + 1)
    longest = jax.random.randint(jax.random.fold_in(key, 1), (MICRO, 1), 0, IMAGES)
    column = jnp.arange(IMAGES)[None, :]
    drawn = jnp.where(column == longest, SEQ_LEN, drawn)
    drawn = jnp.where(column == (longest + 1) % IMAGES, SEQ_LEN // 4, drawn)
    return drawn.astype(jnp.int32)


def steps_of(own_key, dims, shards, least, top_value):
    level, own = 1.0, jax.random.fold_in(own_key, 6)
    for dim, blocks in shards:
        draws = jnp.exp(jax.random.uniform(jax.random.fold_in(own, dim), (blocks,), jnp.float32, least / len(shards), top_value / len(shards)))
        level = level * jnp.repeat(draws, dims[dim] // blocks).reshape([-1 if axis == dim else 1 for axis in range(len(dims))])
    return level


def bell_draw(stream_key, extent, deviation, bound, split=(), dtype=jnp.bfloat16):
    entries = jax.random.normal(stream_key, extent, jnp.float32) * deviation
    if len(split) > 0:
        entries = steps_of(stream_key, extent, split, -0.22, 0.18) * entries
    return jnp.clip(entries, min=-bound, max=bound).astype(dtype)


def setup_inputs(seed: int = 0) -> dict:
    key_of = jax.random.split(jax.random.key(seed), 16)
    tokens = bell_draw(key_of[0], (MICRO, IMAGES, SEQ_LEN, D), 1.0, 6.0, ((1, 4), (2, 4)))
    lengths = draw_lengths(jax.random.fold_in(key_of[15], 71), 0)
    grad_out = bell_draw(key_of[2], (MICRO, IMAGES, SEQ_LEN, D), 1.0, 6.0, ((1, 4), (2, 4)))
    qkv_weight = bell_draw(key_of[3], (3, D, D), D ** -0.5, 0.3125, ((1, 4), (2, 2)), jnp.float32)
    out_weight = bell_draw(key_of[4], (D, D), (D // 16) ** -0.5, 1.25, ((0, 2), (1, 4)), jnp.float32)
    up_weight = bell_draw(key_of[5], (D, FF), D ** -0.5, 0.3125, ((0, 4), (1, 2)), jnp.float32)
    down_weight = bell_draw(key_of[6], (FF, D), FF ** -0.5, 0.15625, ((0, 2), (1, 4)), jnp.float32)
    attn_gain = jnp.clip(1.0 + 0.15 * jax.random.normal(key_of[7], (D,), jnp.float32), 0.25, 1.75)
    ffn_gain = jnp.clip(1.0 + 0.15 * jax.random.normal(key_of[8], (D,), jnp.float32), 0.25, 1.75)
    moment_qkv = bell_draw(key_of[9], (3, D, D), 0.5, 3.0, ((1, 4), (2, 2)), jnp.float32)
    moment_out = bell_draw(key_of[10], (D, D), 0.5, 3.0, ((0, 2), (1, 4)), jnp.float32)
    moment_up = bell_draw(key_of[11], (D, FF), 0.5, 3.0, ((0, 4), (1, 2)), jnp.float32)
    moment_down = bell_draw(key_of[12], (FF, D), 0.5, 3.0, ((0, 2), (1, 4)), jnp.float32)
    moment_attn = bell_draw(key_of[13], (D,), 0.5, 3.0, ((0, 4),), jnp.float32)
    moment_ffn = bell_draw(key_of[14], (D,), 0.5, 3.0, ((0, 4),), jnp.float32)
    return dict(tokens=tokens, lengths=lengths, grad_out=grad_out, qkv_weight=qkv_weight, out_weight=out_weight, up_weight=up_weight, down_weight=down_weight, attn_gain=attn_gain, ffn_gain=ffn_gain, moment_qkv=moment_qkv, moment_out=moment_out, moment_up=moment_up, moment_down=moment_down, moment_attn=moment_attn, moment_ffn=moment_ffn)


def rounded(values):
    return lax.optimization_barrier(values.astype(jnp.bfloat16)).astype(jnp.float32)

def layer_stats(values):
    center = values - lax.optimization_barrier(jnp.mean(values, axis=-1, keepdims=True))
    inv_std = lax.rsqrt(lax.optimization_barrier(jnp.mean(center * center, axis=-1, keepdims=True)) + 1e-06)
    return (center * inv_std, inv_std)

def norm_back(upstream, plain, inv_std, gain):
    scaled = upstream * gain
    return inv_std * (scaled - lax.optimization_barrier(jnp.mean(scaled, axis=-1, keepdims=True)) - plain * lax.optimization_barrier(jnp.mean(scaled * plain, axis=-1, keepdims=True)))

def normal_cdf(values):
    return 0.5 * (1.0 + jax.scipy.special.erf(values * 0.7071067811865476))

def normal_pdf(values):
    return 0.3989422804014327 * jnp.exp(-0.5 * values * values)

def orthogonalize(matrix):
    tall = matrix.shape[0] > matrix.shape[1]
    current = matrix.T if tall else matrix
    current = current / (jnp.sqrt(jnp.sum(current * current)) + 1e-07)
    for sweep in range(NS_STEPS):
        gram = jnp.dot(current, current.T, precision=lax.Precision.HIGHEST)
        poly = -4.775 * gram + 2.0315 * jnp.dot(gram, gram, precision=lax.Precision.HIGHEST)
        current = 3.4445 * current + jnp.dot(poly, current, precision=lax.Precision.HIGHEST)
    return current.T if tall else current

def muon_step(weight, moment):
    ratio = math.sqrt(max(1.0, moment.shape[0] / moment.shape[1]))
    return weight - 0.5 * ratio * orthogonalize(moment)

def block_pass(block_tokens, block_lengths, block_grads, used):
    qkv_use, out_use, up_use, down_use, attn_use, ffn_use = used
    count, length, width = block_tokens.shape
    rows = count * length
    score_scale = HEAD_DIM ** (-0.5)
    f32 = jnp.float32
    bf16 = jnp.bfloat16
    input_rows = block_tokens.reshape(rows, width).astype(f32)
    plain_attn, inv_attn = layer_stats(input_rows)
    norm_attn = (plain_attn * attn_use).astype(bf16)
    query = jnp.dot(norm_attn, qkv_use[0], preferred_element_type=f32).astype(bf16)
    keys = jnp.dot(norm_attn, qkv_use[1], preferred_element_type=f32).astype(bf16)
    values = jnp.dot(norm_attn, qkv_use[2], preferred_element_type=f32).astype(bf16)
    query_h = query.reshape(count, length, HEADS, HEAD_DIM).astype(f32)
    keys_h = keys.reshape(count, length, HEADS, HEAD_DIM).astype(f32)
    values_h = values.reshape(count, length, HEADS, HEAD_DIM).astype(f32)
    valid = lax.broadcasted_iota(jnp.int32, (count, length), 1) < block_lengths[:, None]
    scores = jnp.einsum('bqhe,bkhe->bhqk', query_h, keys_h) * score_scale
    scores = jnp.where(valid[:, None, None, :], scores, -jnp.inf)
    lse = jax.nn.logsumexp(scores, axis=-1, keepdims=True)
    weights = jnp.exp(scores - lse)
    probs = rounded(weights)
    attended = jnp.einsum('bhqk,bkhe->bqhe', probs, values_h).astype(bf16).reshape(rows, width)
    middle = input_rows + jnp.dot(attended, out_use, preferred_element_type=f32)
    plain_ffn, inv_ffn = layer_stats(middle)
    norm_ffn = (plain_ffn * ffn_use).astype(bf16)
    hidden = jnp.dot(norm_ffn, up_use, preferred_element_type=f32)
    activated = (hidden * normal_cdf(hidden)).astype(bf16)
    block_out = (middle + jnp.dot(activated, down_use, preferred_element_type=f32)).astype(bf16)
    upstream = block_grads.reshape(rows, width)
    back_act = jnp.dot(upstream, down_use.T, preferred_element_type=f32)
    back_hidden = (back_act * (normal_cdf(hidden) + hidden * normal_pdf(hidden))).astype(bf16)
    grad_down = jnp.dot(activated.T, upstream, preferred_element_type=f32)
    grad_up = jnp.dot(norm_ffn.T, back_hidden, preferred_element_type=f32)
    back_ffn = jnp.dot(back_hidden, up_use.T, preferred_element_type=f32)
    grad_ffn = lax.optimization_barrier(jnp.sum(back_ffn * plain_ffn, axis=0))
    back_middle = upstream.astype(f32) + norm_back(back_ffn, plain_ffn, inv_ffn, ffn_use)
    middle_half = back_middle.astype(bf16)
    grad_out = jnp.dot(attended.T, middle_half, preferred_element_type=f32)
    back_attended = jnp.dot(middle_half, out_use.T, preferred_element_type=f32).astype(bf16)
    back_heads = back_attended.reshape(count, length, HEADS, HEAD_DIM).astype(f32)
    back_probs = jnp.einsum('bqhe,bkhe->bhqk', back_heads, values_h)
    delta = lax.optimization_barrier(jnp.sum(weights * back_probs, axis=-1, keepdims=True))
    back_scores = rounded(weights * (back_probs - delta) * score_scale)
    back_query = jnp.einsum('bhqk,bkhe->bqhe', back_scores, keys_h).astype(bf16).reshape(rows, width)
    back_keys = jnp.einsum('bhqk,bqhe->bkhe', back_scores, query_h).astype(bf16).reshape(rows, width)
    back_values = jnp.einsum('bhqk,bqhe->bkhe', probs, back_heads).astype(bf16).reshape(rows, width)
    grad_qkv = jnp.stack([jnp.dot(norm_attn.T, back_query, preferred_element_type=f32), jnp.dot(norm_attn.T, back_keys, preferred_element_type=f32), jnp.dot(norm_attn.T, back_values, preferred_element_type=f32)])
    back_attn = jnp.dot(back_query, qkv_use[0].T, preferred_element_type=f32)
    back_attn = back_attn + jnp.dot(back_keys, qkv_use[1].T, preferred_element_type=f32)
    back_attn = back_attn + jnp.dot(back_values, qkv_use[2].T, preferred_element_type=f32)
    grad_attn = lax.optimization_barrier(jnp.sum(back_attn * plain_attn, axis=0))
    input_grad = back_middle + norm_back(back_attn, plain_attn, inv_attn, attn_use)
    grads = (grad_qkv, grad_out, grad_up, grad_down, grad_attn, grad_ffn)
    return (block_out.reshape(block_tokens.shape), input_grad.reshape(block_tokens.shape), grads)

def reference(tokens, lengths, grad_out, qkv_weight, out_weight, up_weight, down_weight, attn_gain, ffn_gain, moment_qkv, moment_out, moment_up, moment_down, moment_attn, moment_ffn):
    f32 = jnp.float32
    bf16 = jnp.bfloat16
    used = (qkv_weight.astype(bf16), out_weight.astype(bf16), up_weight.astype(bf16), down_weight.astype(bf16), rounded(attn_gain), rounded(ffn_gain))
    blocks = MICRO * N_FSDP
    tok_blocks = tokens.reshape(blocks, IMG_DEV, SEQ_LEN, D)
    len_blocks = lengths.reshape(blocks, IMG_DEV)
    grad_blocks = grad_out.reshape(blocks, IMG_DEV, SEQ_LEN, D)

    def scan_step(carry, inputs):
        block_tokens, block_lengths, block_grads = inputs
        block_out, input_grad, grads = block_pass(block_tokens, block_lengths, block_grads, used)
        carry = tuple((total + part for total, part in zip(carry, grads)))
        return (carry, (block_out, input_grad))
    start = (jnp.zeros((3, D, D), f32), jnp.zeros((D, D), f32), jnp.zeros((D, FF), f32), jnp.zeros((FF, D), f32), jnp.zeros((D,), f32), jnp.zeros((D,), f32))
    totals, outputs = lax.scan(scan_step, start, (tok_blocks, len_blocks, grad_blocks))
    block_out = outputs[0].reshape(tokens.shape)
    input_grad = outputs[1].reshape(tokens.shape)
    grad_scale = (MICRO * IMAGES * SEQ_LEN) ** (-0.5)
    qkv_grad, out_grad, up_grad, down_grad, attn_gain_grad, ffn_gain_grad = tuple((total * grad_scale for total in totals))
    new_moment_qkv = 0.5 * moment_qkv + qkv_grad
    new_moment_out = 0.5 * moment_out + out_grad
    new_moment_up = 0.5 * moment_up + up_grad
    new_moment_down = 0.5 * moment_down + down_grad
    new_moment_attn = 0.5 * moment_attn + attn_gain_grad
    new_moment_ffn = 0.5 * moment_ffn + ffn_gain_grad
    new_qkv = jnp.stack([muon_step(qkv_weight[which], new_moment_qkv[which]) for which in range(3)])
    new_out = muon_step(out_weight, new_moment_out)
    new_up = muon_step(up_weight, new_moment_up)
    new_down = muon_step(down_weight, new_moment_down)
    new_attn_gain = attn_gain - 0.3 * new_moment_attn
    new_ffn_gain = ffn_gain - 0.3 * new_moment_ffn
    return (block_out, input_grad, qkv_grad, out_grad, up_grad, down_grad, attn_gain_grad, ffn_gain_grad, new_qkv, new_out, new_up, new_down, new_attn_gain, new_ffn_gain, new_moment_qkv, new_moment_out, new_moment_up, new_moment_down, new_moment_attn, new_moment_ffn)
```

```python
import functools

import jax
import jax.numpy as jnp
from jax import lax
from jax.experimental import pallas as pl
from jax.experimental.pallas import tpu as pltpu
from jax.sharding import PartitionSpec as P

F32 = jnp.float32
BF16 = jnp.bfloat16
MESH = pl.DeviceIdType.MESH
def place():
    rep = lax.axis_size("fsdp") // 4
    fi, s, t = lax.axis_index("fsdp"), lax.axis_index("seq"), lax.axis_index("tp")
    z, fr = fi // rep, lax.rem(fi, rep)
    return rep, z, fr, s, t


def remote(src, dst, ss, rs, dev):
    return pltpu.make_async_remote_copy(src_ref=src, dst_ref=dst, send_sem=ss, recv_sem=rs, device_id=dev, device_id_type=MESH)


def gather_kernel(tok, go, wsh, gsh, w, gains, xo, go_o,
                  zs, zr, pls, plr, pps, ppr, gss, gsr, ts, tr, loc):
    rep, z, fr, s, t = place()
    y, x = s // 2, lax.rem(s, 2)
    zdev = lambda k: {"fsdp": lax.rem(z + k, 4) * rep + fr}
    def sdev(j):
        yy, xx = y, x
        if j & 2: yy = 1 - y
        if j & 1: xx = 1 - x
        return yy * 2 + xx
    other = {"tp": 1 - t}

    bar = pltpu.get_barrier_semaphore()
    for k in range(1, 4):
        pl.semaphore_signal(bar, inc=1, device_id=zdev(k), device_id_type=MESH)
    for j in range(1, 4):
        pl.semaphore_signal(bar, inc=1, device_id={"seq": sdev(j)}, device_id_type=MESH)
    pl.semaphore_signal(bar, inc=1, device_id=other, device_id_type=MESH)
    pl.semaphore_wait(bar, 7)

    def rows(zz, yy=None):
        if yy is None:
            return pl.ds(pl.multiple_of(zz * 96, 32), 96)
        return pl.ds(pl.multiple_of(zz * 96 + yy * 48, 16), 48)
    def cols(tt, xx=None):
        if xx is None:
            return pl.ds(pl.multiple_of(tt * 768, 128), 768)
        return pl.ds(pl.multiple_of(tt * 768 + xx * 384, 128), 384)

    sends = []
    def go_(c):
        c.start(); sends.append(c); return c

    zc = {}
    for m in range(3):
        for k in range(1, 4):
            src = wsh.at[m, pl.ds(pl.multiple_of(y * 48, 16), 48), pl.ds(pl.multiple_of(x * 384, 128), 384)]
            zc[m, k] = go_(remote(src, w.at[m, rows(z, y), cols(t, x)], zs.at[m, k - 1], zr.at[m, k - 1], zdev(k)))
        if m == 0:
            gc = [go_(remote(gsh, gains.at[k], gss.at[k - 1], gsr.at[k - 1], zdev(k))) for k in range(1, 4)]
            tc = []
            for j in range(1, 4):
                for a, (src, dst) in enumerate(((tok, xo), (go, go_o))):
                    tc.append(go_(remote(src.at[sdev(j), t], dst.at[pl.ds(pl.multiple_of(s * 64, 64), 64)], ts.at[a, j - 1], tr.at[a, j - 1], {"seq": sdev(j)})))
    own = []
    for m in range(3):
        own.append(go_(remote(wsh.at[m], w.at[m, rows(z), cols(t)], pps.at[m, 0], ppr.at[m, 0], other)))
    lc = []
    for a, (src, dst) in enumerate(((tok, xo), (go, go_o))):
        lc.append(pltpu.make_async_copy(src.at[s, t], dst.at[pl.ds(pl.multiple_of(s * 64, 64), 64)], loc.at[a]))
    for m in range(3):
        lc.append(pltpu.make_async_copy(wsh.at[m], w.at[m, rows(z), cols(t)], loc.at[2 + m]))
    lc.append(pltpu.make_async_copy(gsh, gains.at[0], loc.at[5]))
    for c in lc:
        c.start()

    pc = {}
    for m in range(3):
        for k in range(1, 4):
            zc[m, k].wait_recv()
            zk = lax.rem(z + 4 - k, 4)
            blk = w.at[m, rows(zk, y), cols(t, x)]
            for j in range(1, 4):
                pc[m, k, j] = go_(remote(blk, blk, pls.at[m, k - 1, j - 1], plr.at[m, k - 1, j - 1], {"seq": sdev(j)}))
    pp = {}
    for m in range(3):
        for k in range(1, 4):
            for j in range(1, 4):
                pc[m, k, j].wait_recv()
            zk = lax.rem(z + 4 - k, 4)
            blk = w.at[m, rows(zk), cols(t)]
            pp[m, k] = go_(remote(blk, blk, pps.at[m, k], ppr.at[m, k], other))
    for m in range(3):
        own[m].wait_recv()
        for k in range(1, 4):
            pp[m, k].wait_recv()
    for c in gc + tc:
        c.wait_recv()
    for c in lc:
        c.wait()
    for c in sends:
        c.wait_send()


def gather(tok, go, wsh, gsh):
    vm = pl.BlockSpec(memory_space=pltpu.VMEM)
    d = wsh.shape[-1] // 2
    D = pltpu.SemaphoreType.DMA
    return pl.pallas_call(
        gather_kernel,
        out_shape=(jax.ShapeDtypeStruct((3, d, 4 * d), BF16), jax.ShapeDtypeStruct((4,) + gsh.shape, BF16),
                   jax.ShapeDtypeStruct((4 * tok.shape[2], d), BF16), jax.ShapeDtypeStruct((4 * tok.shape[2], d), BF16)),
        in_specs=[vm] * 4, out_specs=(vm,) * 4,
        scratch_shapes=[D((3, 3)), D((3, 3)), D((3, 3, 3)), D((3, 3, 3)), D((3, 4)), D((3, 4)), D((3,)), D((3,)), D((2, 3)), D((2, 3)), D((6,))],
        compiler_params=pltpu.CompilerParams(collective_id=0, has_side_effects=True, vmem_limit_bytes=60000 * 1024),
        name="gather",
    )(tok, go, wsh, gsh)


def mm(a, b):
    return jnp.dot(a, b, preferred_element_type=F32)


def mm_nt(a, b):
    return lax.dot_general(a, b, (((1,), (1,)), ((), ())), preferred_element_type=F32)


def mm_tn(a, b):
    return lax.dot_general(a, b, (((0,), (0,)), ((), ())), preferred_element_type=F32)


def stats(v):
    center = v - jnp.mean(v, axis=-1, keepdims=True)
    inv = lax.rsqrt(jnp.mean(center * center, axis=-1, keepdims=True) + 1e-06)
    return center * inv, inv


def norm_back(up, plain, inv, gain):
    e = up * gain
    return inv * (
        e - jnp.mean(e, axis=-1, keepdims=True) - plain * jnp.mean(e * plain, axis=-1, keepdims=True)
    )


def compute_kernel(
    len_ref, x_ref, g_ref, w_ref, gains_ref,
    out_ref, ig_ref, raw_ref, gsum_ref,
    wn, qkv, wts, prb, att, back, natr, raw_n,
):
    length = len_ref[0]
    lanes = lax.broadcasted_iota(jnp.int32, (1, 128), 1)
    low = lanes < 64
    half = 768

    for i, (tile, mixed, first) in enumerate(((0, 2, True), (1, 2, False), (3, 5, True), (4, 5, False))):
        wn[i, :, 0:128] = w_ref[0, :, tile * 128 : tile * 128 + 128]
        wn[i, :, 256:384] = w_ref[0, :, half + tile * 128 : half + tile * 128 + 128]
        a = w_ref[0, :, mixed * 128 : mixed * 128 + 128]
        b = w_ref[0, :, half + mixed * 128 : half + mixed * 128 + 128]
        if first:
            wn[i, :, 128:256] = jnp.where(low, a, b)
        else:
            m = jnp.where(low, b, a).astype(F32)
            wn[i, :, 128:256] = pltpu.roll(m, 64, 1).astype(BF16)

    gains = gains_ref[0].astype(F32)
    for k in range(1, gains_ref.shape[0]):
        gains = gains + gains_ref[k].astype(F32)
    attn_use, ffn_use = gains[0:1], gains[1:2]

    x = x_ref[...].astype(F32)
    plain_attn, inv_attn = stats(x)
    norm_attn = (plain_attn * attn_use).astype(BF16)
    for i in range(3):
        qkv[i] = mm(norm_attn, wn[i]).astype(BF16)
    natr[0] = norm_attn.astype(F32).T.astype(BF16)

    rows = x.shape[0]
    valid = lax.broadcasted_iota(jnp.int32, (rows, 1), 0) < length
    scale = 64 ** (-0.5)

    for p in range(3):
        sl = slice(p * 128, p * 128 + 128)
        q, k, v = qkv[0, :, sl], qkv[1, :, sl], qkv[2, :, sl]
        parts = []
        for h in range(2):
            sel = low if h == 0 else ~low
            s = mm_nt(k, jnp.where(sel, q, jnp.zeros_like(q))) * scale
            s = jnp.where(valid, s, -jnp.inf)
            top = jnp.max(s, axis=0, keepdims=True)
            e = jnp.exp(s - top)
            w = e * (1.0 / jnp.sum(e, axis=0, keepdims=True))
            wts[2 * p + h] = w
            pb = w.astype(BF16)
            prb[2 * p + h] = pb
            parts.append(mm_tn(pb, v))
        att[:, sl] = jnp.where(low, parts[0], parts[1]).astype(BF16)

    middle = x + mm_nt(att[...], wn[3])
    plain_ffn, inv_ffn = stats(middle)
    norm_ffn = (plain_ffn * ffn_use).astype(BF16)
    natr[1] = norm_ffn.astype(F32).T.astype(BF16)
    upstream = g_ref[...]
    natr[2] = upstream.astype(F32).T.astype(BF16)

    acc_out = jnp.zeros((rows, x.shape[1]), F32)
    acc_back = jnp.zeros((rows, x.shape[1]), F32)
    width = 256
    for c in range(1536 // width):
        cs = slice(c * width, c * width + width)
        hidden = mm(norm_ffn, w_ref[1, :, cs])
        cdf = 0.5 * (1.0 + lax.erf(hidden * 0.7071067811865476))
        act = (hidden * cdf).astype(BF16)
        back_act = mm(upstream, w_ref[2, :, cs])
        pdf = 0.3989422804014327 * jnp.exp(-0.5 * hidden * hidden)
        bh = (back_act * (cdf + hidden * pdf)).astype(BF16)
        acc_out = acc_out + mm_nt(act, w_ref[2, :, cs])
        acc_back = acc_back + mm_nt(bh, w_ref[1, :, cs])
        raw_ref[1, :, cs] = mm(natr[1], bh).astype(BF16)
        raw_ref[2, :, cs] = mm(natr[2], act).astype(BF16)
    out_ref[...] = (middle + acc_out).astype(BF16)

    gsum_ref[...] = jnp.zeros_like(gsum_ref)
    gsum_ref[1:2, :] = jnp.sum(acc_back * plain_ffn, axis=0, keepdims=True)
    back_middle = upstream.astype(F32) + norm_back(acc_back, plain_ffn, inv_ffn, ffn_use)
    mh = back_middle.astype(BF16)
    raw_n[3] = mm(back_middle.astype(BF16).astype(F32).T.astype(BF16), att[...]).astype(F32)
    ba = mm(mh, wn[3]).astype(BF16)

    for p in range(3):
        sl = slice(p * 128, p * 128 + 128)
        q, k, v = qkv[0, :, sl], qkv[1, :, sl], qkv[2, :, sl]
        bap = ba[:, sl]
        bq, bk, bv = [], [], []
        for h in range(2):
            sel = low if h == 0 else ~low
            bp = mm_nt(v, jnp.where(sel, bap, jnp.zeros_like(bap)))
            w = wts[2 * p + h]
            delta = jnp.sum(w * bp, axis=0, keepdims=True)
            ds = (w * (bp - delta) * scale).astype(BF16)
            bq.append(mm_tn(ds, k))
            bk.append(mm(ds, q))
            bv.append(mm(prb[2 * p + h], bap))
        back[0, :, sl] = jnp.where(low, bq[0], bq[1]).astype(BF16)
        back[1, :, sl] = jnp.where(low, bk[0], bk[1]).astype(BF16)
        back[2, :, sl] = jnp.where(low, bv[0], bv[1]).astype(BF16)

    back_attn = jnp.zeros((rows, x.shape[1]), F32)
    for i in range(3):
        b = back[i]
        raw_n[i] = mm(natr[0], b)
        back_attn = back_attn + mm_nt(b, wn[i])
    gsum_ref[0:1, :] = jnp.sum(back_attn * plain_attn, axis=0, keepdims=True)
    ig_ref[...] = (back_middle + norm_back(back_attn, plain_attn, inv_attn, attn_use)).astype(BF16)

    for a, b, tile, mixed in ((0, 1, 0, 2), (2, 3, 3, 5)):
        for i, tl in ((a, tile), (b, tile + 1)):
            raw_ref[0, :, tl * 128 : tl * 128 + 128] = raw_n[i, :, 0:128].astype(BF16)
            raw_ref[0, :, half + tl * 128 : half + tl * 128 + 128] = raw_n[i, :, 256:384].astype(BF16)
        first = raw_n[a, :, 128:256]
        second = pltpu.roll(raw_n[b, :, 128:256], 64, 1)
        raw_ref[0, :, mixed * 128 : mixed * 128 + 128] = jnp.where(low, first, second).astype(BF16)
        raw_ref[0, :, half + mixed * 128 : half + mixed * 128 + 128] = jnp.where(low, second, first).astype(BF16)


def compute(length, x, g, w, gains):
    d = x.shape[1]
    rows = x.shape[0]
    vm = pl.BlockSpec(memory_space=pltpu.VMEM)
    return pl.pallas_call(
        compute_kernel,
        out_shape=(
            jax.ShapeDtypeStruct((rows, d), BF16),
            jax.ShapeDtypeStruct((rows, d), BF16),
            jax.ShapeDtypeStruct((3, d, 4 * d), BF16),
            jax.ShapeDtypeStruct((8, d), F32),
        ),
        in_specs=[pl.BlockSpec(memory_space=pltpu.SMEM), vm, vm, vm, vm],
        out_specs=(vm, vm, vm, vm),
        scratch_shapes=[
            pltpu.VMEM((4, d, d), BF16),
            pltpu.VMEM((3, rows, d), BF16),
            pltpu.VMEM((6, rows, rows), F32),
            pltpu.VMEM((6, rows, rows), BF16),
            pltpu.VMEM((rows, d), BF16),
            pltpu.VMEM((3, rows, d), BF16),
            pltpu.VMEM((3, d, rows), BF16),
            pltpu.VMEM((4, d, d), F32),
        ],
        compiler_params=pltpu.CompilerParams(vmem_limit_bytes=60000 * 1024),
        name="image",
    )(length, x, g, w, gains)


def pack_cols(q, k, v, o, t):
    def sp(a):
        if t == 0:
            return a[:, 0:128], a[:, 128:192]
        return a[:, 64:192], a[:, 0:64]
    (qp, q2), (kp, k2), (vp, v2), (op, o2) = sp(q), sp(k), sp(v), sp(o)
    if t == 0:
        return jnp.concatenate([qp, kp, q2, k2, vp, op, v2, o2], axis=1)
    return jnp.concatenate([qp, kp, k2, q2, vp, op, o2, v2], axis=1)


def unpack_cols(a, t):
    c = lambda lo, n: a[:, lo : lo + n]
    if t == 0:
        q = jnp.concatenate([c(0, 128), c(256, 64)], 1)
        k = jnp.concatenate([c(128, 128), c(320, 64)], 1)
        v = jnp.concatenate([c(384, 128), c(640, 64)], 1)
        o = jnp.concatenate([c(512, 128), c(704, 64)], 1)
    else:
        q = jnp.concatenate([c(320, 64), c(0, 128)], 1)
        k = jnp.concatenate([c(256, 64), c(128, 128)], 1)
        v = jnp.concatenate([c(704, 64), c(384, 128)], 1)
        o = jnp.concatenate([c(640, 64), c(512, 128)], 1)
    return q, k, v, o


def split(a):
    hi = a.astype(BF16)
    return hi, (a - hi.astype(F32)).astype(BF16)


def dot3(a, b):
    (ah, al), (bh, bl) = a, b
    return mm(ah, bh) + (mm(ah, bl) + mm(al, bh))


def dot3c(a, b):
    (ah, al), (bh, bl) = a, b
    return mm(jnp.concatenate([ah, ah, al], 1), jnp.concatenate([bh, bl, bh], 0))


def ns(m_ref, d_ref, q_hi, q_lo, d3):
    m = m_ref[...]
    gram = mm_nt(m, m)
    n = gram.shape[0]
    eye = lax.broadcasted_iota(jnp.int32, (n, n), 0) == lax.broadcasted_iota(jnp.int32, (n, n), 1)
    total = jnp.sum(jnp.where(eye, gram, 0.0))
    inv = 1.0 / (jnp.sqrt(total) + 1e-07)
    gram = gram * (inv * inv)
    ident = jnp.where(eye, 3.4445, 0.0)

    def poly(gs, gram):
        return ident + (-4.775 * gram + 2.0315 * d3(gs, gs))
    q = None
    for it in range(5):
        gs = split(gram)
        r = poly(gs, gram)
        rs = split(r)
        q = r if q is None else d3(rs, split(q))
        if it < 4:
            gram = d3(split(d3(rs, rs)), gs)
    qh, ql = split(q)
    q_hi[...] = qh
    q_lo[...] = ql
    for c in range(0, m_ref.shape[1], 256):
        cs = slice(c, c + 256)
        d_ref[:, cs] = ((mm(q_hi[...], m_ref[:, cs]) + mm(q_lo[...], m_ref[:, cs])) * inv).astype(BF16)


def run(m, which):
    d3 = {'3': dot3, 'c': dot3c}[which]
    vm = pl.BlockSpec(memory_space=pltpu.VMEM)
    return pl.pallas_call(lambda *r: ns(*r, d3), out_shape=jax.ShapeDtypeStruct(m.shape, BF16), in_specs=[vm], out_specs=vm,
      scratch_shapes=[pltpu.VMEM((m.shape[0],)*2, BF16)]*2, compiler_params=pltpu.CompilerParams(vmem_limit_bytes=60000*1024), name="ns")(m)


OWNERS = ((1, 0, 0), (2, 3, 0), (1, 1, 0), (2, 1, 0), (1, 2, 0), (2, 2, 0))
def newton_schulz(role, mbuf, dbuf, q_hi, q_lo):
    wide = (role == 0) | (role == 1)
    first = (role == 2) | (role == 4)
    col = lax.broadcasted_iota(jnp.int32, (1, mbuf.shape[1]), 1)
    right = col >= 384
    cc = jnp.where(right, col - 384, col)
    lead = (cc < 128) | ((cc >= 256) & (jnp.where(right, 1, 0) == jnp.where(cc >= 320, 1, 0)))
    pick = jnp.where(lead, 1, 0)
    keep = jnp.where(wide, 1, jnp.where(col >= 768, 0, jnp.where(first, pick, 1 - pick)))
    zero = jnp.zeros((), BF16)
    n = mbuf.shape[0]
    gram = jnp.zeros((n, n), F32)
    for c in range(0, mbuf.shape[1], 512):
        m = jnp.where(keep[:, c : c + 512] > 0, mbuf[:, c : c + 512], zero)
        mbuf[:, c : c + 512] = m
        gram = gram + mm_nt(m, m)
    eye = lax.broadcasted_iota(jnp.int32, (n, n), 0) == lax.broadcasted_iota(jnp.int32, (n, n), 1)
    inv = 1.0 / (jnp.sqrt(jnp.sum(jnp.where(eye, gram, 0.0))) + 1e-07)
    gram = gram * (inv * inv)
    ident = jnp.where(eye, 3.4445, 0.0)
    q = None
    for it in range(5):
        gs = split(gram)
        r = ident + (-4.775 * gram + 2.0315 * dot3c(gs, gs))
        rs = split(r)
        q = r if q is None else dot3c(rs, split(q))
        if it < 4:
            gram = dot3c(split(dot3c(rs, rs)), gs)
    qh, ql = split(q)
    q_hi[...] = qh
    q_lo[...] = ql
    fac = inv * jnp.where(role == 1, 1.0, 0.5)
    for c in range(0, mbuf.shape[1], 256):
        m = mbuf[:, c : c + 256]
        dbuf[:, c : c + 256] = ((mm(q_hi[...], m) + mm(q_lo[...], m)) * fac).astype(BF16)


def reduce_kernel(scale, raw, gs, mom, bo, ig,
                  grad_sh, delta_sh, bo_out, ig_out, gs_out,
                  pr, acc, sx, xr, sy, yr, sz, zr, mb, mbuf, dbuf, dpc, q_hi, q_lo, g1, g2, g3, gz, gst,
                  ps_s, ps_r, x_s, x_r, y_s, y_r, z_s, z_r, a_s, a_r, o_s, m_r, d_s, d_r, e_s, e_r, t_s, t_r, g_s, g_r, loc):
    rep, z, fr, s, t = place()
    y, x = s // 2, lax.rem(s, 2)
    def zdev(k):
        return {"fsdp": lax.rem(z + k, 4) * rep + fr}
    def sidx(j):
        yy, xx = y, x
        if j & 2: yy = 1 - y
        if j & 1: xx = 1 - x
        return yy * 2 + xx
    def sdev(j):
        return {"seq": sidx(j)}
    other = {"tp": 1 - t}
    me = z * 8 + s * 2 + t
    def dev(i):
        return {"fsdp": (i // 8) * rep + fr, "seq": lax.rem(i // 2, 4), "tp": lax.rem(i, 2)}

    bar = pltpu.get_barrier_semaphore()
    def greet(i, carry):
        pl.semaphore_signal(bar, inc=1, device_id=dev(lax.rem(me + i, 32)), device_id_type=MESH)
        return carry
    lax.fori_loop(1, 32, greet, 0)
    pl.semaphore_wait(bar, 31)

    r48 = lambda yy: pl.ds(pl.multiple_of(yy * 48, 16), 48)
    r96 = lambda zz, yy: pl.ds(pl.multiple_of(zz * 96 + yy * 48, 16), 48)
    c384 = lambda xx: pl.ds(pl.multiple_of(xx * 384, 128), 384)
    c768 = lambda tt: pl.ds(pl.multiple_of(tt * 768, 128), 768)

    sends = []
    def go(c):
        c.start()
        sends.append(c)
        return c

    order = (1, 2, 0)
    pc = {m: go(remote(raw.at[m, :, c768(1 - t)], pr.at[m], ps_s.at[m], ps_r.at[m], other)) for m in order}
    gc = go(remote(gs, g1, g_s.at[0], g_r.at[0], other))
    xc = {}
    for m in order:
        pc[m].wait_recv()
        theirs = pl.ds(pl.multiple_of(t * 768 + (1 - x) * 384, 128), 384)
        sx[m] = (raw[m, :, theirs].astype(F32) + pr[m, :, c384(1 - x)].astype(F32)).astype(BF16)
        xc[m] = go(remote(sx.at[m], xr.at[m], x_s.at[m], x_r.at[m], sdev(1)))
        mine = pl.ds(pl.multiple_of(t * 768 + x * 384, 128), 384)
        acc[m] = raw[m, :, mine].astype(F32) + pr[m, :, c384(x)].astype(F32)
    gc.wait_recv()
    gst[0] = gs[...] + g1[...]
    gc = go(remote(gst.at[0], g2, g_s.at[1], g_r.at[1], sdev(1)))
    yc = {}
    for m in order:
        xc[m].wait_recv()
        for f in range(4):
            rr = pl.ds(pl.multiple_of(f * 96 + (1 - y) * 48, 16), 48)
            sy[m, f] = (acc[m, rr, :] + xr[m, rr, :].astype(F32)).astype(BF16)
        yc[m] = go(remote(sy.at[m], yr.at[m], y_s.at[m], y_r.at[m], sdev(2)))
        for f in range(4):
            rr = pl.ds(pl.multiple_of(f * 96 + y * 48, 16), 48)
            acc[m, rr, :] = acc[m, rr, :] + xr[m, rr, :].astype(F32)
    gc.wait_recv()
    gst[1] = gst[0] + g2[...]
    gc = go(remote(gst.at[1], g3, g_s.at[2], g_r.at[2], sdev(2)))
    zc = {}
    for m in order:
        yc[m].wait_recv()
        for k in range(1, 4):
            zk = lax.rem(z + k, 4)
            sz[m, k - 1] = (acc[m, r96(zk, y), :] + yr[m, zk].astype(F32)).astype(BF16)
            zc[m, k] = go(remote(sz.at[m, k - 1], zr.at[m, k - 1], z_s.at[m, k - 1], z_r.at[m, k - 1], zdev(k)))
    gc.wait_recv()
    gz[pl.ds(z, 1)] = (gst[1] + g3[...])[None]
    gcs = []
    for k in range(1, 4):
        gcs.append(go(remote(gz.at[z], gz.at[z], g_s.at[2 + k], g_r.at[2 + k], zdev(k))))

    def owner_dev(o):
        zo, so, to = OWNERS[o]
        return {"fsdp": zo * rep + fr, "seq": so, "tp": to}
    def am(o):
        zo, so, to = OWNERS[o]
        return (z == zo) & (s == so) & (t == to)

    def piece(src, o, dst, i, cond=None):
        mine = am(o)
        far = ~mine if cond is None else (~mine) & cond
        near = mine if cond is None else mine & cond
        @pl.when(far)
        def _():
            remote(src, dst, o_s.at[i], m_r.at[me], owner_dev(o)).start()
        @pl.when(near)
        def _():
            pltpu.make_async_copy(src, dst, m_r.at[me]).start()
        def fin():
            @pl.when(far)
            def _():
                remote(src, dst, o_s.at[i], m_r.at[me], owner_dev(o)).wait_send()
        return fin

    fins = []
    ac = []
    for m in order:
        tot = acc[m, r96(z, y), :] + yr[m, z].astype(F32)
        for k in range(1, 4):
            zc[m, k].wait_recv()
            tot = tot + zr[m, k - 1].astype(F32)
        grad_sh[m, r48(y), c384(x)] = (tot * scale).astype(BF16)
        blk = grad_sh.at[m, r48(y), c384(x)]
        gb = grad_sh[m, r48(y), c384(x)].astype(F32)
        mb[m] = (0.5 * mom[m, r48(y), c384(x)] + gb).astype(BF16)
        wide = mbuf.at[r96(z, y), pl.ds(pl.multiple_of(t * 768 + x * 384, 128), 384)]
        narrow = mbuf.at[r96(z, y), c384(t)]
        if m == 1:
            fins.append(piece(mb.at[m], 0, wide, 0))
        elif m == 2:
            fins.append(piece(mb.at[m], 1, wide, 1))
        else:
            fins.append(piece(mb.at[m], 2, narrow, 2, x == 0))
            fins.append(piece(mb.at[m], 3, narrow, 3, x == 0))
            fins.append(piece(mb.at[m], 4, narrow, 2, x == 1))
            fins.append(piece(mb.at[m], 5, narrow, 3, x == 1))
        for j in range(1, 4):
            ac.append(go(remote(blk, blk, a_s.at[m, j - 1], a_r.at[m, j - 1], sdev(j))))
    for k in range(1, 4):
        gcs[k - 1].wait_recv()
    gs_out[...] = ((gz[0] + gz[1]) + (gz[2] + gz[3])) * scale

    lc = []
    for a, (src, dst) in enumerate(((bo, bo_out), (ig, ig_out))):
        for j in range(4):
            sj = sidx(j)
            blk = src.at[pl.ds(pl.multiple_of(sj * 64, 64), 64)]
            if j:
                go(remote(blk, dst.at[s, t], t_s.at[a, j, 0], t_r.at[a, j, 0], {"seq": sj}))
            else:
                lc.append(pltpu.make_async_copy(blk, dst.at[s, t], loc.at[a]))
                lc[-1].start()
            go(remote(blk, dst.at[s, t], t_s.at[a, j, 1], t_r.at[a, j, 1], {"seq": sj, "tp": 1 - t}))

    role = jnp.int32(-1)
    for o in range(6):
        role = jnp.where(am(o), o, role)
    slot = jnp.where(role == 0, 1, jnp.where(role == 1, 2, jnp.where((role == 2) | (role == 4), 0, 3)))
    xo = jnp.where(role >= 4, 1, 0)

    def involved(i):
        return (role < 2) | (lax.rem(i // 2, 2) == xo)

    def own_region(ref, i):
        zz, ss, tt = i // 8, lax.rem(i // 2, 4), lax.rem(i, 2)
        yy, xx = ss // 2, lax.rem(ss, 2)
        start = jnp.where(role < 2, tt * 768 + xx * 384, tt * 384)
        return ref.at[pl.ds(pl.multiple_of(zz * 96 + yy * 48, 16), 48), pl.ds(pl.multiple_of(start, 128), 384)]

    @pl.when(role >= 0)
    def _():
        def arrive(i, carry):
            @pl.when(involved(i))
            def _():
                reg = own_region(mbuf, i)
                pltpu.make_async_copy(mb.at[0], reg, m_r.at[i]).wait()
            return carry
        @pl.when(role >= 2)
        def _():
            mbuf[:, 768:1536] = jnp.zeros((mbuf.shape[0], 768), BF16)
        lax.fori_loop(0, 32, arrive, 0)
        newton_schulz(role, mbuf, dbuf, q_hi, q_lo)
        def leave(i, carry):
            reg = own_region(dbuf, i)
            @pl.when(involved(i) & (i != me))
            def _():
                remote(reg, dpc.at[slot], d_s.at[i], d_r.at[slot], dev(i)).start()
            @pl.when(involved(i) & (i == me))
            def _():
                pltpu.make_async_copy(reg, dpc.at[slot], d_r.at[slot]).start()
            return carry
        lax.fori_loop(0, 32, leave, 0)

    ec = []
    def got(i):
        pltpu.make_async_copy(mb.at[0], dpc.at[i], d_r.at[i]).wait()
    for m in order:
        if m:
            got(m)
            delta_sh[m, r48(y), c384(x)] = dpc[m]
        else:
            got(0)
            got(3)
            cc = lax.broadcasted_iota(jnp.int32, (1, 384), 1)
            lead = (cc < 128) | ((cc >= 256) & (t == jnp.where(cc >= 320, 1, 0)))
            delta_sh[m, r48(y), c384(x)] = jnp.where(lead, dpc[0], dpc[3])
        blk = delta_sh.at[m, r48(y), c384(x)]
        for j in range(1, 4):
            ec.append(go(remote(blk, blk, e_s.at[m, j - 1], e_r.at[m, j - 1], sdev(j))))
    for c in ac + ec:
        c.wait_recv()
    for a, (src, dst) in enumerate(((bo, bo_out), (ig, ig_out))):
        for j in range(4):
            sj = sidx(j)
            blk = src.at[pl.ds(0, 64)]
            if j:
                remote(blk, dst.at[sj, t], t_s.at[a, j, 0], t_r.at[a, j, 0], {"seq": sj}).wait_recv()
            remote(blk, dst.at[sj, 1 - t], t_s.at[a, j, 1], t_r.at[a, j, 1], {"seq": sj, "tp": 1 - t}).wait_recv()
    for c in lc:
        c.wait()
    for c in sends:
        c.wait_send()
    for f in fins:
        f()
    @pl.when(role >= 0)
    def _():
        def done(i, carry):
            @pl.when(involved(i) & (i != me))
            def _():
                remote(own_region(dbuf, i), dpc.at[slot], d_s.at[i], d_r.at[slot], dev(i)).wait_send()
            return carry
        lax.fori_loop(0, 32, done, 0)


def reduce(scale, raw, gs, mom, bo, ig):
    vm = pl.BlockSpec(memory_space=pltpu.VMEM)
    d = raw.shape[1]
    D = pltpu.SemaphoreType.DMA
    V = pltpu.VMEM
    rows = bo.shape[0] // 4
    return pl.pallas_call(
        functools.partial(reduce_kernel, scale),
        out_shape=(
            jax.ShapeDtypeStruct((3, 96, 768), BF16),
            jax.ShapeDtypeStruct((3, 96, 768), BF16),
            jax.ShapeDtypeStruct((4, 2, rows, d), BF16),
            jax.ShapeDtypeStruct((4, 2, rows, d), BF16),
            jax.ShapeDtypeStruct((8, d), F32),
        ),
        in_specs=[vm] * 5, out_specs=(vm,) * 5,
        scratch_shapes=[
            V((3, 384, 768), BF16), V((3, 384, 384), F32), V((3, 384, 384), BF16), V((3, 384, 384), BF16),
            V((3, 4, 48, 384), BF16), V((3, 4, 48, 384), BF16), V((3, 3, 48, 384), BF16), V((3, 3, 48, 384), BF16),
            V((3, 48, 384), BF16), V((384, 1536), BF16), V((384, 1536), BF16), V((4, 48, 384), BF16),
            V((384, 384), BF16), V((384, 384), BF16),
            V((8, d), F32), V((8, d), F32), V((8, d), F32), V((4, 8, d), F32), V((2, 8, d), F32),
            D((3,)), D((3,)), D((3,)), D((3,)), D((3,)), D((3,)), D((3, 3)), D((3, 3)), D((3, 3)), D((3, 3)),
            D((4,)), D((32,)), D((32,)), D((4,)), D((3, 3)), D((3, 3)), D((2, 4, 2)), D((2, 4, 2)), D((6,)), D((6,)), D((2,)),
        ],
        compiler_params=pltpu.CompilerParams(collective_id=1, has_side_effects=True, vmem_limit_bytes=60000 * 1024),
        name="reduce",
    )(raw, gs, mom, bo, ig)


def cols(a, lo, n):
    return a[..., lo : lo + n]


def pack(q, k, v, o, t):
    even = jnp.concatenate([cols(q, 0, 128), cols(k, 0, 128), cols(q, 128, 64), cols(k, 128, 64),
                            cols(v, 0, 128), cols(o, 0, 128), cols(v, 128, 64), cols(o, 128, 64)], axis=-1)
    odd = jnp.concatenate([cols(q, 64, 128), cols(k, 64, 128), cols(k, 0, 64), cols(q, 0, 64),
                           cols(v, 64, 128), cols(o, 64, 128), cols(o, 0, 64), cols(v, 0, 64)], axis=-1)
    return jnp.where(t == 0, even, odd)


def unpack(a, t):
    def two(big, first, second):
        even = jnp.concatenate([cols(a, big, 128), cols(a, first, 64)], -1)
        odd = jnp.concatenate([cols(a, second, 64), cols(a, big, 128)], -1)
        return jnp.where(t == 0, even, odd)
    return two(0, 256, 320), two(128, 320, 256), two(384, 640, 704), two(512, 704, 640)


def body(tokens, lengths, grad_out, qkv_weight, out_weight, up_weight, down_weight, attn_gain, ffn_gain,
         moment_qkv, moment_out, moment_up, moment_down, moment_attn, moment_ffn):
    micro, img_dev, tok_loc, width = tokens.shape
    fsdp = lax.axis_size("fsdp")
    rep = fsdp // 4
    fi, s, t = lax.axis_index("fsdp"), lax.axis_index("seq"), lax.axis_index("tp")
    z, fr = fi // rep, lax.rem(fi, rep)
    full = tok_loc * lax.axis_size("seq")
    scale = (micro * img_dev * fsdp * full) ** (-0.5)
    groups = [[a * rep + b for b in range(rep)] for a in range(4)]

    def packed(qkv, out, up, down):
        return jnp.stack([pack(qkv[0], qkv[1], qkv[2], out.T, t), up, down.T])

    def widen(a, axis):
        return a if rep == 1 else lax.all_gather(a, "fsdp", axis=axis, tiled=True, axis_index_groups=groups)

    wsh = widen(packed(qkv_weight, out_weight, up_weight, down_weight).astype(BF16), 1)
    mom = widen(packed(moment_qkv, moment_out, moment_up, moment_down), 1)
    gains = widen(jnp.stack([attn_gain, ffn_gain]).astype(BF16), 1)
    gsh = lax.dynamic_update_slice(jnp.zeros((16, width), BF16), gains, (0, z * gains.shape[1]))

    w, gains, x, g = gather(tokens, grad_out, wsh, gsh)
    length = lax.dynamic_slice(lengths, (s, t), (1, 1)).reshape(1)
    bo, ig, raw, gsum = compute(length, x, g, w, gains)
    if rep > 1:
        rgroups = groups
        raw = lax.psum(raw.astype(F32), "fsdp", axis_index_groups=rgroups).astype(BF16)
        gsum = lax.psum(gsum, "fsdp", axis_index_groups=rgroups)
    grad, delta, bo, ig, gsum = reduce(scale, raw, gsum, mom, bo, ig)

    def narrow(a):
        n = qkv_weight.shape[1]
        return a if rep == 1 else lax.dynamic_slice_in_dim(a, fr * n, n, axis=1)

    grad = narrow(grad).astype(F32)
    delta = narrow(delta).astype(F32)
    def parts(a):
        q, k, v, o = unpack(a[0], t)
        return jnp.stack([q, k, v]), o.T, a[1], a[2].T
    gq, go, gu, gd = parts(grad)
    dq, do, du, dd = parts(delta)
    n = attn_gain.shape[0]
    ga, gf = lax.dynamic_slice(gsum, (0, fi * n), (2, n))
    mq, mo, mu, md = 0.5 * moment_qkv + gq, 0.5 * moment_out + go, 0.5 * moment_up + gu, 0.5 * moment_down + gd
    ma, mf = 0.5 * moment_attn + ga, 0.5 * moment_ffn + gf
    return (bo, ig.astype(F32), gq, go, gu, gd, ga, gf,
            qkv_weight - dq, out_weight - do, up_weight - du, down_weight - dd,
            attn_gain - 0.3 * ma, ffn_gain - 0.3 * mf, mq, mo, mu, md, ma, mf)


def solution(mesh):
    weights = (P(None, "fsdp", "tp"), P("tp", "fsdp"), P("fsdp", "tp"), P("tp", "fsdp"), P("fsdp"), P("fsdp"))
    rows = P(None, "fsdp", "seq", None)
    return jax.shard_map(body, mesh=mesh, in_specs=(rows, P(None, "fsdp"), rows) + weights + weights,
                         out_specs=(rows, rows) + weights + weights + weights, check_vma=False)
```

```python
import functools

import jax
import jax.numpy as jnp
from jax import lax
from jax.experimental import pallas as pl
from jax.experimental.pallas import tpu as pltpu
from jax.sharding import PartitionSpec as P

F32 = jnp.float32
BF16 = jnp.bfloat16
MESH = pl.DeviceIdType.MESH
def place():
    rep = lax.axis_size("fsdp") // 4
    fi, s, t = lax.axis_index("fsdp"), lax.axis_index("seq"), lax.axis_index("tp")
    z, fr = fi // rep, lax.rem(fi, rep)
    return rep, z, fr, s, t


def remote(src, dst, ss, rs, dev):
    return pltpu.make_async_remote_copy(src_ref=src, dst_ref=dst, send_sem=ss, recv_sem=rs, device_id=dev, device_id_type=MESH)


def mm(a, b):
    return jnp.dot(a, b, preferred_element_type=F32)


def mm_nt(a, b):
    return lax.dot_general(a, b, (((1,), (1,)), ((), ())), preferred_element_type=F32)


def mm_tn(a, b):
    return lax.dot_general(a, b, (((0,), (0,)), ((), ())), preferred_element_type=F32)


def stats(v):
    center = v - jnp.mean(v, axis=-1, keepdims=True)
    inv = lax.rsqrt(jnp.mean(center * center, axis=-1, keepdims=True) + 1e-06)
    return center * inv, inv


def norm_back(up, plain, inv, gain):
    e = up * gain
    return inv * (
        e - jnp.mean(e, axis=-1, keepdims=True) - plain * jnp.mean(e * plain, axis=-1, keepdims=True)
    )


def split(a):
    hi = a.astype(BF16)
    return hi, (a - hi.astype(F32)).astype(BF16)


def dot3c(a, b):
    (ah, al), (bh, bl) = a, b
    return mm(jnp.concatenate([ah, ah, al], 1), jnp.concatenate([bh, bl, bh], 0))


OWNERS = ((1, 0, 0), (2, 3, 0), (1, 1, 0), (2, 1, 0), (1, 2, 0), (2, 2, 0))
def newton_schulz(role, mbuf, dbuf, q_hi, q_lo):
    wide = (role == 0) | (role == 1)
    first = (role == 2) | (role == 4)
    col = lax.broadcasted_iota(jnp.int32, (1, mbuf.shape[1]), 1)
    right = col >= 384
    cc = jnp.where(right, col - 384, col)
    lead = (cc < 128) | ((cc >= 256) & (jnp.where(right, 1, 0) == jnp.where(cc >= 320, 1, 0)))
    pick = jnp.where(lead, 1, 0)
    keep = jnp.where(wide, 1, jnp.where(col >= 768, 0, jnp.where(first, pick, 1 - pick)))
    zero = jnp.zeros((), BF16)
    n = mbuf.shape[0]
    gram = jnp.zeros((n, n), F32)
    for c in range(0, mbuf.shape[1], 512):
        m = jnp.where(keep[:, c : c + 512] > 0, mbuf[:, c : c + 512], zero)
        mbuf[:, c : c + 512] = m
        gram = gram + mm_nt(m, m)
    eye = lax.broadcasted_iota(jnp.int32, (n, n), 0) == lax.broadcasted_iota(jnp.int32, (n, n), 1)
    inv = 1.0 / (jnp.sqrt(jnp.sum(jnp.where(eye, gram, 0.0))) + 1e-07)
    gram = gram * (inv * inv)
    ident = jnp.where(eye, 3.4445, 0.0)
    q = None
    for it in range(5):
        gs = split(gram)
        r = ident + (-4.775 * gram + 2.0315 * dot3c(gs, gs))
        rs = split(r)
        q = r if q is None else dot3c(rs, split(q))
        if it < 4:
            gram = dot3c(split(dot3c(rs, rs)), gs)
    qh, ql = split(q)
    q_hi[...] = qh
    q_lo[...] = ql
    fac = inv * jnp.where(role == 1, 1.0, 0.5)
    for c in range(0, mbuf.shape[1], 256):
        m = mbuf[:, c : c + 256]
        dbuf[:, c : c + 256] = ((mm(q_hi[...], m) + mm(q_lo[...], m)) * fac).astype(BF16)


def put_cols(dst, tile, mixed, spare, a, t):
    @pl.when(t == 0)
    def _():
        dst[:, tile * 128 : tile * 128 + 128] = a[:, 0:128]
        dst[:, mixed * 128 + 64 * spare : mixed * 128 + 64 * spare + 64] = a[:, 128:192]
    @pl.when(t == 1)
    def _():
        dst[:, tile * 128 : tile * 128 + 128] = a[:, 64:192]
        dst[:, mixed * 128 + 64 * (1 - spare) : mixed * 128 + 64 * (1 - spare) + 64] = a[:, 0:64]


SPOTS = ((0, 2, 0), (1, 2, 1), (3, 5, 0), (4, 5, 1))
def get_cols(a, tile, mixed, spare, t):
    big = a[:, tile * 128 : tile * 128 + 128]
    lo = a[:, mixed * 128 + 64 * spare : mixed * 128 + 64 * spare + 64]
    hi = a[:, mixed * 128 + 64 * (1 - spare) : mixed * 128 + 64 * (1 - spare) + 64]
    return jnp.where(t == 0, jnp.concatenate([big, lo], 1), jnp.concatenate([hi, big], 1))


def pack_kernel(qkv, out, up, down, mqkv, mout, mup, mdown, ga, gf, wsh, msh, gv, tmp):
    t = lax.axis_index("tp")
    for a, b, c, d, dst in ((qkv, out, up, down, wsh), (mqkv, mout, mup, mdown, msh)):
        dt = dst.dtype
        view = tmp
        for i in range(3):
            put_cols(view, *SPOTS[i], a[i], t)
        put_cols(view, *SPOTS[3], b[...].T, t)
        dst[0] = tmp[...].astype(dt)
        dst[1] = c[...].astype(dt)
        dst[2] = d[...].astype(dt)
    n = ga.shape[1]
    rows = jnp.concatenate([ga[...], gf[...], jnp.zeros((14, n), F32)], 0)
    gv[...] = jnp.concatenate([rows, jnp.zeros((16, 128 - n), F32)], 1).astype(BF16)


def pack(*args):
    vm = pl.BlockSpec(memory_space=pltpu.VMEM)
    return pl.pallas_call(
        pack_kernel,
        out_shape=(jax.ShapeDtypeStruct((3, 96, 768), BF16), jax.ShapeDtypeStruct((3, 96, 768), F32), jax.ShapeDtypeStruct((16, 128), BF16)),
        in_specs=[vm] * 10, out_specs=(vm,) * 3,
        scratch_shapes=[pltpu.VMEM((96, 768), F32)],
        name="pack",
    )(*args)


def epilogue_kernel(grad, delta, gs, bo, ig, qkv, out, up, down, ga, gf, mqkv, mout, mup, mdown, ma, mf,
                    bo_o, ig_o, gqkv, gout, gup, gdown, gga, ggf, nqkv, nout, nup, ndown, nga, ngf,
                    nmqkv, nmout, nmup, nmdown, nma, nmf):
    rep = lax.axis_size("fsdp") // 4
    z, t = lax.axis_index("fsdp") // rep, lax.axis_index("tp")
    bo_o[...] = bo[...]
    ig_o[...] = ig[...].astype(F32)
    def one(g, d, w, m, g_o, w_o, m_o):
        g_o[...] = g
        new = 0.5 * m[...] + g
        m_o[...] = new
        w_o[...] = w[...] - d
    g0, d0 = grad[0].astype(F32), delta[0].astype(F32)
    for i in range(3):
        one(get_cols(g0, *SPOTS[i], t), get_cols(d0, *SPOTS[i], t), qkv.at[i], mqkv.at[i], gqkv.at[i], nqkv.at[i], nmqkv.at[i])
    one(get_cols(g0, *SPOTS[3], t).T, get_cols(d0, *SPOTS[3], t).T, out, mout, gout, nout, nmout)
    one(grad[1].astype(F32), delta[1].astype(F32), up, mup, gup, nup, nmup)
    one(grad[2].astype(F32), delta[2].astype(F32), down, mdown, gdown, ndown, nmdown)
    n = ga.shape[1]
    for row, (w, m, g_o, w_o, m_o) in enumerate(((ga, ma, gga, nga, nma), (gf, mf, ggf, ngf, nmf))):
        for zz in range(4):
            @pl.when(z == zz)
            def _():
                g_o[...] = gs[row : row + 1, zz * n : zz * n + n]
        new = 0.5 * m[...] + g_o[...]
        m_o[...] = new
        w_o[...] = w[...] - 0.3 * new


def epilogue(grad, delta, gs, bo, ig, w, m):
    vm = pl.BlockSpec(memory_space=pltpu.VMEM)
    sd = lambda a: jax.ShapeDtypeStruct(a.shape, F32)
    ws = tuple(sd(a) for a in w)
    return pl.pallas_call(
        epilogue_kernel,
        out_shape=(jax.ShapeDtypeStruct(bo.shape, BF16), sd(ig)) + ws * 3,
        in_specs=[vm] * 17, out_specs=(vm,) * 20,
        name="epilogue",
    )(grad, delta, gs, bo, ig, *w, *m)


UNITS = ((1, 0, 4, True), (2, 0, 4, False), (0, 0, 2, True), (0, 2, 2, False))
def whole_kernel(scale, shapes, names, *refs):
    r = dict(zip(names, refs))
    rep, z, fr, s, t = place()
    y, x = s // 2, lax.rem(s, 2)
    me = z * 8 + s * 2 + t
    other = {"tp": 1 - t}

    def zdev(k):
        return {"fsdp": lax.rem(z + k, 4) * rep + fr}

    def sidx(j):
        yy, xx = y, x
        if j & 2:
            yy = 1 - y
        if j & 1:
            xx = 1 - x
        return yy * 2 + xx

    def sdev(j):
        return {"seq": sidx(j)}

    def dev(i):
        return {"fsdp": (i // 8) * rep + fr, "seq": lax.rem(i // 2, 4), "tp": lax.rem(i, 2)}

    def al(v, n):
        return pl.multiple_of(v, n)

    def rows(zz, yy=None):
        return pl.ds(al(zz * 96, 32), 96) if yy is None else pl.ds(al(zz * 96 + yy * 48, 16), 48)

    def cols(tt, xx=None):
        return pl.ds(al(tt * 768, 128), 768) if xx is None else pl.ds(al(tt * 768 + xx * 384, 128), 384)

    def r48(yy):
        return pl.ds(al(yy * 48, 16), 48)

    def c384(xx):
        return pl.ds(al(xx * 384, 128), 384)

    bar = pltpu.get_barrier_semaphore()

    def greet(i, carry):
        pl.semaphore_signal(bar, inc=1, device_id=dev(lax.rem(me + i, 32)), device_id_type=MESH)
        return carry

    lax.fori_loop(1, 32, greet, 0)
    for b in range(1, rep):
        pl.semaphore_signal(bar, inc=1, device_id={"fsdp": z * rep + lax.rem(fr + b, rep)}, device_id_type=MESH)
    pl.semaphore_wait(bar, 31 + rep - 1)

    sends = []

    def go(c):
        c.start()
        sends.append(c)
        return c

    w, wsh = r["w"], r["wsh"]
    order = (0, 1, 2)
    zc, pc, pp, own = {}, {}, {}, {}
    locs = []

    def keep(c):
        c.start()
        locs.append(c)
        return c

    for m in order:
        for k in range(1, 4):
            src = wsh.at[m, r48(y), c384(x)]
            zc[m, k] = go(remote(src, w.at[m, rows(z, y), cols(t, x)], r["w_zs"].at[m, k - 1], r["w_zr"].at[m, k - 1], zdev(k)))
        if m == 0:
            gc = [go(remote(r["gv"], r["gains"].at[z], r["gv_s"].at[k - 1], r["gv_r"].at[k - 1], zdev(k))) for k in range(1, 4)]
    tc = []
    seg = pl.ds(al(s * 64, 64), 64)
    for a, (src, dst) in enumerate(((r["tok"], r["xin"]), (r["cot"], r["gin"]))):
        for j in range(1, 4):
            tc.append(go(remote(src.at[sidx(j), t], dst.at[seg], r["t_s"].at[a, j - 1], r["t_r"].at[a, j - 1], sdev(j))))
        keep(pltpu.make_async_copy(src.at[s, t], dst.at[seg], r["loc"].at[a]))
    for m in order:
        own[m] = go(remote(wsh.at[m], w.at[m, rows(z), cols(t)], r["w_ps"].at[m, 0], r["w_pr"].at[m, 0], other))
        keep(pltpu.make_async_copy(wsh.at[m], w.at[m, rows(z), cols(t)], r["loc"].at[2 + m]))
    keep(pltpu.make_async_copy(r["gv"], r["gains"].at[z], r["loc"].at[5]))

    def chunk(m, k, j):
        zk = lax.rem(z + 4 - k, 4)
        sj = sidx(j)
        return w.at[m, rows(zk, sj // 2), cols(t, lax.rem(sj, 2))]

    def plane(m):
        for k in range(1, 4):
            zc[m, k].wait_recv()
            blk = chunk(m, k, 0)
            for j in (1, 2):
                pc[m, k, j] = go(remote(blk, blk, r["w_ls"].at[m, k - 1, j - 1], r["w_lr"].at[m, k - 1, j - 1], sdev(j)))

    def relay(m):
        for k in range(1, 4):
            via = 1 + (m + k) % 2
            pc[m, k, via].wait_recv()
            blk = chunk(m, k, via)
            pc[m, k, 3] = go(remote(blk, blk, r["w_ls"].at[m, k - 1, 2], r["w_lr"].at[m, k - 1, 2], sdev(3 - via)))

    def across(m):
        for k in range(1, 4):
            pc[m, k, 2 - (m + k) % 2].wait_recv()
            pc[m, k, 3].wait_recv()
            blk = w.at[m, rows(lax.rem(z + 4 - k, 4)), cols(t)]
            pp[m, k] = go(remote(blk, blk, r["w_ps"].at[m, k], r["w_pr"].at[m, k], other))

    def landed(m):
        own[m].wait_recv()
        for k in range(1, 4):
            pp[m, k].wait_recv()

    plane(0)
    relay(0)
    plane(1)
    across(0)
    for c in tc[:3]:
        c.wait_recv()
    for c in locs:
        c.wait()
    for c in gc:
        c.wait_recv()

    length = r["len"][0]
    lanes = lax.broadcasted_iota(jnp.int32, (1, 128), 1)
    low = lanes < 64
    half = 768
    wn, qkv, wts, prb, att, back, natr = (r[n] for n in ("wn", "qkv", "wts", "prb", "att", "back", "natr"))
    raw, gsum = r["raw"], r["gsum"]
    gfull = r["gfull"]
    n = 96
    for zz in range(4):
        gfull[:, zz * n : zz * n + n] = r["gains"][zz, 0:8, 0:n].astype(F32)
    attn_use, ffn_use = gfull[0:1, :], gfull[1:2, :]

    xin = r["xin"][...].astype(F32)
    plain_attn, inv_attn = stats(xin)
    norm_attn = (plain_attn * attn_use).astype(BF16)
    natr[0] = norm_attn.astype(F32).T.astype(BF16)
    relay(1)
    landed(0)
    for i, (tile, mixed, first) in enumerate(((0, 2, True), (1, 2, False), (3, 5, True), (4, 5, False))):
        wn[i, :, 0:128] = w[0, :, tile * 128 : tile * 128 + 128]
        wn[i, :, 256:384] = w[0, :, half + tile * 128 : half + tile * 128 + 128]
        a = w[0, :, mixed * 128 : mixed * 128 + 128]
        b = w[0, :, half + mixed * 128 : half + mixed * 128 + 128]
        if first:
            wn[i, :, 128:256] = jnp.where(low, a, b)
        else:
            wn[i, :, 128:256] = pltpu.roll(jnp.where(low, b, a).astype(F32), 64, 1).astype(BF16)
    for i in range(3):
        qkv[i] = mm(norm_attn, wn[i]).astype(BF16)
    plane(2)
    nrow = xin.shape[0]
    valid = lax.broadcasted_iota(jnp.int32, (nrow, 1), 0) < length
    hscale = 64 ** (-0.5)
    for p in range(3):
        sl = slice(p * 128, p * 128 + 128)
        q, k, v = qkv[0, :, sl], qkv[1, :, sl], qkv[2, :, sl]
        parts = []
        for h in range(2):
            sel = low if h == 0 else ~low
            sc = mm_nt(k, jnp.where(sel, q, jnp.zeros_like(q))) * hscale
            sc = jnp.where(valid, sc, -jnp.inf)
            e = jnp.exp(sc - jnp.max(sc, axis=0, keepdims=True))
            wt = e * (1.0 / jnp.sum(e, axis=0, keepdims=True))
            wts[2 * p + h] = wt
            pb = wt.astype(BF16)
            prb[2 * p + h] = pb
            parts.append(mm_tn(pb, v))
        att[:, sl] = jnp.where(low, parts[0], parts[1]).astype(BF16)
        if p == 0:
            across(1)
        if p == 1:
            relay(2)
    middle = xin + mm_nt(att[...], wn[3])
    plain_ffn, inv_ffn = stats(middle)
    norm_ffn = (plain_ffn * ffn_use).astype(BF16)
    natr[1] = norm_ffn.astype(F32).T.astype(BF16)
    for c in tc[3:]:
        c.wait_recv()
    upstream = r["gin"][...]
    natr[2] = upstream.astype(F32).T.astype(BF16)
    across(2)
    landed(1)
    landed(2)

    prx = r["prx"]
    pair = {}

    def send_pair(m):
        pair[m] = go(remote(raw.at[m, :, cols(1 - t)], prx.at[m], r["p_s"].at[m], r["p_r"].at[m], other))

    first, second = {}, {}

    def stage_first(u):
        m, f0, nf, xfirst = UNITS[u]
        rr = slice(f0 * 96, f0 * 96 + nf * 96)
        fs, fo = r["fs%d" % u], r["fo%d" % u]
        if xfirst:
            fs[...] = (raw[m, rr, cols(t, 1 - x)].astype(F32) + prx[m, rr, c384(1 - x)].astype(F32)).astype(BF16)
            fo[...] = raw[m, rr, cols(t, x)].astype(F32) + prx[m, rr, c384(x)].astype(F32)
        else:
            for f in range(nf):
                far = pl.ds(al((f0 + f) * 96 + (1 - y) * 48, 16), 48)
                near = pl.ds(al((f0 + f) * 96 + y * 48, 16), 48)
                fs[f] = (raw[m, far, cols(t)].astype(F32) + prx[m, far, :].astype(F32)).astype(BF16)
                fo[f] = raw[m, near, cols(t)].astype(F32) + prx[m, near, :].astype(F32)
        first[u] = go(remote(fs, r["fr%d" % u], r["f_s"].at[u], r["f_r"].at[u], sdev(1 if xfirst else 2)))

    part = r["part"]

    def stage_second(u):
        m, f0, nf, xfirst = UNITS[u]
        first[u].wait_recv()
        fo, fr_, ss = r["fo%d" % u], r["fr%d" % u], r["ss%d" % u]
        for f in range(nf):
            if xfirst:
                far = pl.ds(al(f * 96 + (1 - y) * 48, 16), 48)
                near = pl.ds(al(f * 96 + y * 48, 16), 48)
                ss[f] = (fo[far, :] + fr_[far, :].astype(F32)).astype(BF16)
                part[m, f0 + f] = fo[near, :] + fr_[near, :].astype(F32)
            else:
                ss[f] = (fo[f, :, c384(1 - x)] + fr_[f, :, c384(1 - x)].astype(F32)).astype(BF16)
                part[m, f0 + f] = fo[f, :, c384(x)] + fr_[f, :, c384(x)].astype(F32)
        second[u] = go(remote(ss, r["sr%d" % u], r["s_s"].at[u], r["s_r"].at[u], sdev(2 if xfirst else 1)))

    gz = {}

    def stage_z(m):
        for u, (mu, f0, nf, xfirst) in enumerate(UNITS):
            if mu == m:
                second[u].wait_recv()
                for f in range(nf):
                    part[m, f0 + f] = part[m, f0 + f] + r["sr%d" % u][f].astype(F32)
        for k in range(1, 4):
            r["zs"][m, k - 1] = part[m, lax.rem(z + k, 4)].astype(BF16)
            gz[m, k] = go(remote(r["zs"].at[m, k - 1], r["zr"].at[m, k - 1], r["z_s"].at[m, k - 1], r["z_r"].at[m, k - 1], zdev(k)))

    def owner_dev(o):
        zo, so, to = OWNERS[o]
        return {"fsdp": zo * rep + fr, "seq": so, "tp": to}

    def am(o):
        zo, so, to = OWNERS[o]
        return (z == zo) & (s == so) & (t == to)

    fins = []
    mbuf, dbuf, dpc, mb = r["mbuf"], r["dbuf"], r["dpc"], r["mb"]

    def piece(src, o, dst, i, cond=None):
        mine = am(o)
        far = ~mine if cond is None else (~mine) & cond
        near = mine if cond is None else mine & cond

        @pl.when(far)
        def _():
            remote(src, dst, r["o_s"].at[i], r["m_r"].at[me], owner_dev(o)).start()

        @pl.when(near)
        def _():
            pltpu.make_async_copy(src, dst, r["m_r"].at[me]).start()

        def fin():
            @pl.when(far)
            def _():
                remote(src, dst, r["o_s"].at[i], r["m_r"].at[me], owner_dev(o)).wait_send()

        fins.append(fin)

    ac = []
    grad_sh, delta_sh, mom = r["grad_sh"], r["delta_sh"], r["mom"]

    def stage_final(m):
        tot = part[m, z]
        for k in range(1, 4):
            gz[m, k].wait_recv()
            tot = tot + r["zr"][m, k - 1].astype(F32)
        if rep > 1:
            r["rs"][m] = tot.astype(BF16)
            rc = [go(remote(r["rs"].at[m], r["rr"].at[m, b - 1], r["r_s"].at[m, b - 1], r["r_r"].at[m, b - 1], {"fsdp": z * rep + lax.rem(fr + b, rep)})) for b in range(1, rep)]
            for b in range(1, rep):
                rc[b - 1].wait_recv()
                tot = tot + r["rr"][m, b - 1].astype(F32)
        half_g = (tot * scale).astype(BF16)
        grad_sh[m, r48(y), c384(x)] = half_g
        mb[m] = (0.5 * mom[m, r48(y), c384(x)] + half_g.astype(F32)).astype(BF16)
        wide = mbuf.at[rows(z, y), cols(t, x)]
        slim = mbuf.at[rows(z, y), c384(t)]
        if m:
            piece(mb.at[m], m - 1, wide, m - 1)
        else:
            piece(mb.at[m], 2, slim, 2, x == 0)
            piece(mb.at[m], 3, slim, 3, x == 0)
            piece(mb.at[m], 4, slim, 2, x == 1)
            piece(mb.at[m], 5, slim, 3, x == 1)
        blk = grad_sh.at[m, r48(y), c384(x)]
        for j in range(1, 4):
            ac.append(go(remote(blk, blk, r["a_s"].at[m, j - 1], r["a_r"].at[m, j - 1], sdev(j))))

    def images(a, src, dst):
        for j in range(4):
            sj = sidx(j)
            blk = src.at[pl.ds(al(sj * 64, 64), 64)]
            if j:
                go(remote(blk, dst.at[s, t], r["i_s"].at[a, j, 0], r["i_r"].at[a, j, 0], {"seq": sj}))
            else:
                keep(pltpu.make_async_copy(blk, dst.at[s, t], r["loc"].at[6 + a]))
            go(remote(blk, dst.at[s, t], r["i_s"].at[a, j, 1], r["i_r"].at[a, j, 1], {"seq": sj, "tp": 1 - t}))

    acc_out = jnp.zeros(xin.shape, F32)
    acc_back = jnp.zeros(xin.shape, F32)
    width = 256
    for c in range(1536 // width):
        cs = slice(c * width, c * width + width)
        hidden = mm(norm_ffn, w[1, :, cs])
        cdf = 0.5 * (1.0 + lax.erf(hidden * 0.7071067811865476))
        act = (hidden * cdf).astype(BF16)
        back_act = mm(upstream, w[2, :, cs])
        pdf = 0.3989422804014327 * jnp.exp(-0.5 * hidden * hidden)
        bh = (back_act * (cdf + hidden * pdf)).astype(BF16)
        acc_out = acc_out + mm_nt(act, w[2, :, cs])
        acc_back = acc_back + mm_nt(bh, w[1, :, cs])
        raw[1, :, cs] = mm(natr[1], bh).astype(BF16)
        raw[2, :, cs] = mm(natr[2], act).astype(BF16)
    send_pair(1)
    send_pair(2)
    r["bo"][...] = (middle + acc_out).astype(BF16)
    gsum[...] = jnp.zeros_like(gsum)
    gsum[1:2, :] = jnp.sum(acc_back * plain_ffn, axis=0, keepdims=True)
    back_middle = upstream.astype(F32) + norm_back(acc_back, plain_ffn, inv_ffn, ffn_use)
    mh = back_middle.astype(BF16)
    ba = mm(mh, wn[3]).astype(BF16)

    raw_n = r["raw_n"]
    for p in range(3):
        sl = slice(p * 128, p * 128 + 128)
        q, k, v = qkv[0, :, sl], qkv[1, :, sl], qkv[2, :, sl]
        bap = ba[:, sl]
        bq, bk, bv = [], [], []
        for h in range(2):
            sel = low if h == 0 else ~low
            bp = mm_nt(v, jnp.where(sel, bap, jnp.zeros_like(bap)))
            wt = wts[2 * p + h]
            dl = jnp.sum(wt * bp, axis=0, keepdims=True)
            ds = (wt * (bp - dl) * hscale).astype(BF16)
            bq.append(mm_tn(ds, k))
            bk.append(mm(ds, q))
            bv.append(mm(prb[2 * p + h], bap))
        back[0, :, sl] = jnp.where(low, bq[0], bq[1]).astype(BF16)
        back[1, :, sl] = jnp.where(low, bk[0], bk[1]).astype(BF16)
        back[2, :, sl] = jnp.where(low, bv[0], bv[1]).astype(BF16)
        if p == 0:
            pair[1].wait_recv()
            stage_first(0)
        if p == 1:
            pair[2].wait_recv()
            stage_first(1)
    for i in range(3):
        raw_n[i] = mm(natr[0], back[i])
    raw_n[3] = mm(mh.astype(F32).T.astype(BF16), att[...])
    for a, b, tile, mixed in ((0, 1, 0, 2), (2, 3, 3, 5)):
        for i, tl in ((a, tile), (b, tile + 1)):
            raw[0, :, tl * 128 : tl * 128 + 128] = raw_n[i, :, 0:128].astype(BF16)
            raw[0, :, half + tl * 128 : half + tl * 128 + 128] = raw_n[i, :, 256:384].astype(BF16)
        lead = raw_n[a, :, 128:256]
        tail = pltpu.roll(raw_n[b, :, 128:256], 64, 1)
        raw[0, :, mixed * 128 : mixed * 128 + 128] = jnp.where(low, lead, tail).astype(BF16)
        raw[0, :, half + mixed * 128 : half + mixed * 128 + 128] = jnp.where(low, tail, lead).astype(BF16)
    send_pair(0)
    stage_second(0)
    back_attn = jnp.zeros(xin.shape, F32)
    for i in range(3):
        back_attn = back_attn + mm_nt(back[i], wn[i])
    gsum[0:1, :] = jnp.sum(back_attn * plain_attn, axis=0, keepdims=True)
    gc = go(remote(gsum, r["g1"], r["g_s"].at[0], r["g_r"].at[0], other))
    pair[0].wait_recv()
    stage_first(2)
    stage_first(3)
    stage_second(1)
    r["ig"][...] = (back_middle + norm_back(back_attn, plain_attn, inv_attn, attn_use)).astype(BF16)
    gst, gzz = r["gst"], r["gzz"]
    gc.wait_recv()
    gst[0] = gsum[...] + r["g1"][...]
    gc = go(remote(gst.at[0], r["g2"], r["g_s"].at[1], r["g_r"].at[1], sdev(1)))
    stage_z(1)
    stage_second(2)
    stage_second(3)
    stage_z(2)
    gc.wait_recv()
    gst[1] = gst[0] + r["g2"][...]
    gc = go(remote(gst.at[1], r["g3"], r["g_s"].at[2], r["g_r"].at[2], sdev(2)))
    stage_final(1)
    stage_z(0)
    stage_final(2)
    stage_final(0)
    gc.wait_recv()
    gzz[pl.ds(z, 1)] = (gst[1] + r["g3"][...])[None]
    gcs = [go(remote(gzz.at[z], gzz.at[z], r["g_s"].at[2 + k], r["g_r"].at[2 + k], zdev(k))) for k in range(1, 4)]
    images(0, r["bo"], r["bo_out"])
    images(1, r["ig"], r["ig_out"])
    for c in gcs:
        c.wait_recv()
    gtot = (gzz[0] + gzz[1]) + (gzz[2] + gzz[3])
    if rep > 1:
        r["grs"][pl.ds(fr, 1)] = gtot[None]
        grc = [go(remote(r["grs"].at[fr], r["grs"].at[fr], r["gr_s"].at[b - 1], r["gr_r"].at[b - 1], {"fsdp": z * rep + lax.rem(fr + b, rep)})) for b in range(1, rep)]
        for c in grc:
            c.wait_recv()
        gtot = r["grs"][0]
        for b in range(1, rep):
            gtot = gtot + r["grs"][b]
    r["gs_out"][...] = gtot * scale

    role = jnp.int32(-1)
    for o in range(6):
        role = jnp.where(am(o), o, role)
    slot = jnp.where(role == 0, 1, jnp.where(role == 1, 2, jnp.where((role == 2) | (role == 4), 0, 3)))
    xo = jnp.where(role >= 4, 1, 0)

    def involved(i):
        return (role < 2) | (lax.rem(i // 2, 2) == xo)

    def region(ref, i):
        zz, ss, tt = i // 8, lax.rem(i // 2, 4), lax.rem(i, 2)
        yy, xx = ss // 2, lax.rem(ss, 2)
        start = jnp.where(role < 2, tt * 768 + xx * 384, tt * 384)
        return ref.at[rows(zz, yy), pl.ds(al(start, 128), 384)]

    @pl.when(role >= 0)
    def _():
        def arrive(i, carry):
            @pl.when(involved(i))
            def _():
                pltpu.make_async_copy(mb.at[0], region(mbuf, i), r["m_r"].at[i]).wait()
            return carry

        @pl.when(role >= 2)
        def _():
            mbuf[:, 768:1536] = jnp.zeros((mbuf.shape[0], 768), BF16)

        lax.fori_loop(0, 32, arrive, 0)
        newton_schulz(role, mbuf, dbuf, r["q_hi"], r["q_lo"])

        def leave(i, carry):
            reg = region(dbuf, i)

            @pl.when(involved(i) & (i != me))
            def _():
                remote(reg, dpc.at[slot], r["d_s"].at[i], r["d_r"].at[slot], dev(i)).start()

            @pl.when(involved(i) & (i == me))
            def _():
                pltpu.make_async_copy(reg, dpc.at[slot], r["d_r"].at[slot]).start()
            return carry

        lax.fori_loop(0, 32, leave, 0)

    ec = []
    for m in (1, 2, 0):
        for i in ((m,) if m else (0, 3)):
            pltpu.make_async_copy(mb.at[0], dpc.at[i], r["d_r"].at[i]).wait()
        if m:
            delta_sh[m, r48(y), c384(x)] = dpc[m]
        else:
            cc = lax.broadcasted_iota(jnp.int32, (1, 384), 1)
            lead = (cc < 128) | ((cc >= 256) & (t == jnp.where(cc >= 320, 1, 0)))
            delta_sh[m, r48(y), c384(x)] = jnp.where(lead, dpc[0], dpc[3])
        blk = delta_sh.at[m, r48(y), c384(x)]
        for j in range(1, 4):
            ec.append(go(remote(blk, blk, r["e_s"].at[m, j - 1], r["e_r"].at[m, j - 1], sdev(j))))
    for c in ac + ec:
        c.wait_recv()
    for a, (src, dst) in enumerate(((r["bo"], r["bo_out"]), (r["ig"], r["ig_out"]))):
        for j in range(4):
            sj = sidx(j)
            blk = src.at[pl.ds(0, 64)]
            if j:
                remote(blk, dst.at[sj, t], r["i_s"].at[a, j, 0], r["i_r"].at[a, j, 0], {"seq": sj}).wait_recv()
            remote(blk, dst.at[sj, 1 - t], r["i_s"].at[a, j, 1], r["i_r"].at[a, j, 1], {"seq": sj, "tp": 1 - t}).wait_recv()
    for c in locs[6:]:
        c.wait()
    for c in sends:
        c.wait_send()
    for f in fins:
        f()

    @pl.when(role >= 0)
    def _():
        def done(i, carry):
            @pl.when(involved(i) & (i != me))
            def _():
                remote(region(dbuf, i), dpc.at[slot], r["d_s"].at[i], r["d_r"].at[slot], dev(i)).wait_send()
            return carry

        lax.fori_loop(0, 32, done, 0)


def whole(scale, rep, length, tok, cot, wsh, mom, gv):
    vm = pl.BlockSpec(memory_space=pltpu.VMEM)
    D = pltpu.SemaphoreType.DMA
    V = pltpu.VMEM
    d = tok.shape[-1]
    seg = tok.shape[2]
    n = 4 * seg
    ins = ["len", "tok", "cot", "wsh", "mom", "gv"]
    outs = {
        "grad_sh": ((3, 96, 768), BF16), "delta_sh": ((3, 96, 768), BF16),
        "bo_out": ((4, 2, seg, d), BF16), "ig_out": ((4, 2, seg, d), BF16), "gs_out": ((8, d), F32),
    }
    scr = {
        "w": V((3, d, 4 * d), BF16), "gains": V((4, 16, 128), BF16), "gfull": V((8, d), F32),
        "xin": V((n, d), BF16), "gin": V((n, d), BF16),
        "wn": V((4, d, d), BF16), "qkv": V((3, n, d), BF16), "wts": V((6, n, n), F32), "prb": V((6, n, n), BF16),
        "att": V((n, d), BF16), "back": V((3, n, d), BF16), "natr": V((3, d, n), BF16), "raw_n": V((4, d, d), F32),
        "raw": V((3, d, 4 * d), BF16), "gsum": V((8, d), F32), "bo": V((n, d), BF16), "ig": V((n, d), BF16),
        "prx": V((3, d, 768), BF16), "part": V((3, 4, 48, 384), F32),
        "zs": V((3, 3, 48, 384), BF16), "zr": V((3, 3, 48, 384), BF16), "mb": V((3, 48, 384), BF16),
        "mbuf": V((384, 1536), BF16), "dbuf": V((384, 1536), BF16), "dpc": V((4, 48, 384), BF16),
        "q_hi": V((384, 384), BF16), "q_lo": V((384, 384), BF16),
        "g1": V((8, d), F32), "g2": V((8, d), F32), "g3": V((8, d), F32), "gzz": V((4, 8, d), F32), "gst": V((2, 8, d), F32),
        "w_zs": D((3, 3)), "w_zr": D((3, 3)), "w_ls": D((3, 3, 3)), "w_lr": D((3, 3, 3)), "w_ps": D((3, 4)), "w_pr": D((3, 4)),
        "gv_s": D((3,)), "gv_r": D((3,)), "t_s": D((2, 3)), "t_r": D((2, 3)), "loc": D((8,)),
        "p_s": D((3,)), "p_r": D((3,)), "f_s": D((4,)), "f_r": D((4,)), "s_s": D((4,)), "s_r": D((4,)),
        "z_s": D((3, 3)), "z_r": D((3, 3)), "a_s": D((3, 3)), "a_r": D((3, 3)), "o_s": D((4,)), "m_r": D((32,)),
        "d_s": D((32,)), "d_r": D((4,)), "e_s": D((3, 3)), "e_r": D((3, 3)), "i_s": D((2, 4, 2)), "i_r": D((2, 4, 2)),
        "g_s": D((6,)), "g_r": D((6,)),
    }
    for u, (m, f0, nf, xfirst) in enumerate(UNITS):
        a = (nf * 96, 384) if xfirst else (nf, 48, 768)
        scr["fs%d" % u] = V(a, BF16)
        scr["fr%d" % u] = V(a, BF16)
        scr["fo%d" % u] = V(a, F32)
        scr["ss%d" % u] = V((nf, 48, 384), BF16)
        scr["sr%d" % u] = V((nf, 48, 384), BF16)
    if rep > 1:
        scr.update({"rs": V((3, 48, 384), BF16), "rr": V((3, rep - 1, 48, 384), BF16), "r_s": D((3, rep - 1)), "r_r": D((3, rep - 1)),
                    "grs": V((rep, 8, d), F32), "gr_s": D((rep - 1,)), "gr_r": D((rep - 1,))})
    names = ins + list(outs) + list(scr)
    return pl.pallas_call(
        functools.partial(whole_kernel, scale, None, names),
        out_shape=tuple(jax.ShapeDtypeStruct(*o) for o in outs.values()),
        in_specs=[pl.BlockSpec(memory_space=pltpu.SMEM)] + [vm] * 5, out_specs=(vm,) * 5,
        scratch_shapes=list(scr.values()),
        compiler_params=pltpu.CompilerParams(collective_id=0, has_side_effects=True, vmem_limit_bytes=60 * 1024 * 1024),
        name="whole",
    )(length, tok, cot, wsh, mom, gv)


def body(tokens, lengths, grad_out, *params):
    micro, img_dev, tok_loc, width = tokens.shape
    fsdp = lax.axis_size("fsdp")
    rep = fsdp // 4
    fi, s, t = lax.axis_index("fsdp"), lax.axis_index("seq"), lax.axis_index("tp")
    scale = (micro * img_dev * fsdp * tok_loc * lax.axis_size("seq")) ** (-0.5)
    groups = [[a * rep + b for b in range(rep)] for a in range(4)]
    split_dims = (1, 1, 0, 1, 0, 0)

    def ready(values):
        if rep > 1:
            values = [lax.all_gather(a, "fsdp", axis=d, tiled=True, axis_index_groups=groups) for a, d in zip(values, split_dims)]
        qkv, out, up, down, ga, gf = values
        return [qkv, out, up, down.T, ga[None], gf[None]]

    def done(values):
        qkv, out, up, down, ga, gf = values
        values = [qkv, out, up, down.T, ga[0], gf[0]]
        if rep > 1:
            fr = lax.rem(fi, rep)
            values = [lax.dynamic_slice_in_dim(a, fr * (a.shape[d] // rep), a.shape[d] // rep, axis=d) for a, d in zip(values, split_dims)]
        return values

    w, m = ready(params[:6]), ready(params[6:])
    wsh, mom, gv = pack(*w[:4], *m[:4], w[4], w[5])
    length = lax.dynamic_slice(lengths, (s, t), (1, 1)).reshape(1)
    grad, delta, bo, ig, gs = whole(scale, rep, length, tokens, grad_out, wsh, mom, gv)
    o = epilogue(grad, delta, gs, bo, ig, w, m)
    return tuple(o[:2]) + tuple(done(o[2:8])) + tuple(done(o[8:14])) + tuple(done(o[14:]))


def solution(mesh):
    weights = (P(None, "fsdp", "tp"), P("tp", "fsdp"), P("fsdp", "tp"), P("tp", "fsdp"), P("fsdp"), P("fsdp"))
    rows = P(None, "fsdp", "seq", None)
    return jax.shard_map(body, mesh=mesh, in_specs=(rows, P(None, "fsdp"), rows) + weights + weights,
                         out_specs=(rows, rows) + weights + weights + weights, check_vma=False)
```

```python
import functools

import jax
import jax.numpy as jnp
from jax import lax
from jax.experimental import pallas as pl
from jax.experimental.pallas import tpu as pltpu
from jax.sharding import PartitionSpec as P

F32 = jnp.float32
BF16 = jnp.bfloat16
MESH = pl.DeviceIdType.MESH
def place():
    rep = lax.axis_size("fsdp") // 4
    fi, s, t = lax.axis_index("fsdp"), lax.axis_index("seq"), lax.axis_index("tp")
    z, fr = fi // rep, lax.rem(fi, rep)
    return rep, z, fr, s, t


def remote(src, dst, ss, rs, dev):
    return pltpu.make_async_remote_copy(src_ref=src, dst_ref=dst, send_sem=ss, recv_sem=rs, device_id=dev, device_id_type=MESH)


def mm(a, b):
    return jnp.dot(a, b, preferred_element_type=F32)


def mm_nt(a, b):
    return lax.dot_general(a, b, (((1,), (1,)), ((), ())), preferred_element_type=F32)


def mm_tn(a, b):
    return lax.dot_general(a, b, (((0,), (0,)), ((), ())), preferred_element_type=F32)


def stats(v):
    center = v - jnp.mean(v, axis=-1, keepdims=True)
    inv = lax.rsqrt(jnp.mean(center * center, axis=-1, keepdims=True) + 1e-06)
    return center * inv, inv


def norm_back(up, plain, inv, gain):
    e = up * gain
    return inv * (
        e - jnp.mean(e, axis=-1, keepdims=True) - plain * jnp.mean(e * plain, axis=-1, keepdims=True)
    )


def split(a):
    hi = a.astype(BF16)
    return hi, (a - hi.astype(F32)).astype(BF16)


def dot3c(a, b):
    (ah, al), (bh, bl) = a, b
    return mm(jnp.concatenate([ah, ah, al], 1), jnp.concatenate([bh, bl, bh], 0))


def newton_schulz(z, s, t, mbuf, da, dw, gbox):
    n = mbuf.shape[0]

    @pl.when(t == 1)
    def _():
        gram = jnp.zeros((n, n), F32)
        for c in range(0, mbuf.shape[1], 512):
            m = mbuf[:, c : c + 512]
            gram = gram + mm_nt(m, m)
        gbox[...] = gram

    @pl.when(t == 0)
    def _():
        high = lax.broadcasted_iota(jnp.int32, (1, 128), 1) >= 64
        second = s // 2
        for tt in range(2):
            keep = jnp.where(high, 1, 0) == (1 - second if tt else second)
            cs = slice(tt * 256 + 128, tt * 256 + 256)
            m = mbuf[:, cs]
            mbuf[:, cs] = jnp.where(keep, m, jnp.zeros_like(m))
        m = mbuf[:, 0:512]
        gbox[...] = mm_nt(m, m)

    gram = gbox[...]
    eye = lax.broadcasted_iota(jnp.int32, (n, n), 0) == lax.broadcasted_iota(jnp.int32, (n, n), 1)
    inv = 1.0 / (jnp.sqrt(jnp.sum(jnp.where(eye, gram, 0.0))) + 1e-07)
    gram = gram * (inv * inv)
    ident = jnp.where(eye, 3.4445, 0.0)
    q = None
    for it in range(5):
        gs = split(gram)
        if it < 4:
            r = ident + (-4.775 * gram + 2.0315 * dot3c(gs, gs))
            rs = split(r)
            if q is None:
                gbox[...] = r
                q = gbox[pl.ds(pl.multiple_of(z * 96, 32), 96), :]
            else:
                q = dot3c(split(q), rs)
            gram = dot3c(split(dot3c(rs, rs)), gs)
        else:
            one = dot3c(split(q), gs)
            q = 3.4445 * q + (-4.775 * one + 2.0315 * dot3c(split(one), gs))
    qh, ql = split(q)

    @pl.when(t == 1)
    def _():
        fac = inv * jnp.where(s >= 2, 1.0, 0.5)
        for c in range(0, 768, 256):
            m = mbuf[:, pl.ds(pl.multiple_of(lax.rem(s, 2) * 768 + c, 256), 256)]
            dw[:, c : c + 256] = ((mm(qh, m) + mm(ql, m)) * fac).astype(BF16)

    @pl.when(t == 0)
    def _():
        for tt in range(2):
            m = mbuf[:, tt * 256 : tt * 256 + 256]
            da[tt] = ((mm(qh, m) + mm(ql, m)) * (inv * 0.5)).astype(BF16)


def put_cols(dst, tile, mixed, spare, a, t):
    @pl.when(t == 0)
    def _():
        dst[:, tile * 128 : tile * 128 + 128] = a[:, 0:128]
        dst[:, mixed * 128 + 64 * spare : mixed * 128 + 64 * spare + 64] = a[:, 128:192]
    @pl.when(t == 1)
    def _():
        dst[:, tile * 128 : tile * 128 + 128] = a[:, 64:192]
        dst[:, mixed * 128 + 64 * (1 - spare) : mixed * 128 + 64 * (1 - spare) + 64] = a[:, 0:64]


SPOTS = ((0, 2, 0), (1, 2, 1), (3, 5, 0), (4, 5, 1))
def get_cols(a, tile, mixed, spare, t):
    big = a[:, tile * 128 : tile * 128 + 128]
    lo = a[:, mixed * 128 + 64 * spare : mixed * 128 + 64 * spare + 64]
    hi = a[:, mixed * 128 + 64 * (1 - spare) : mixed * 128 + 64 * (1 - spare) + 64]
    return jnp.where(t == 0, jnp.concatenate([big, lo], 1), jnp.concatenate([hi, big], 1))


def epilogue_kernel(grad, delta, gs, bo, ig, qkv, out, up, down, ga, gf, mqkv, mout, mup, mdown, ma, mf,
                    bo_o, ig_o, gqkv, gout, gup, gdown, gga, ggf, nqkv, nout, nup, ndown, nga, ngf,
                    nmqkv, nmout, nmup, nmdown, nma, nmf):
    rep = lax.axis_size("fsdp") // 4
    z, t = lax.axis_index("fsdp") // rep, lax.axis_index("tp")
    bo_o[...] = bo[...]
    ig_o[...] = ig[...].astype(F32)
    def one(g, d, w, m, g_o, w_o, m_o):
        g_o[...] = g
        new = 0.5 * m[...] + g
        m_o[...] = new
        w_o[...] = w[...] - d
    g0, d0 = grad[0].astype(F32), delta[0].astype(F32)
    for i in range(3):
        one(get_cols(g0, *SPOTS[i], t), get_cols(d0, *SPOTS[i], t), qkv.at[i], mqkv.at[i], gqkv.at[i], nqkv.at[i], nmqkv.at[i])
    one(get_cols(g0, *SPOTS[3], t).T, get_cols(d0, *SPOTS[3], t).T, out, mout, gout, nout, nmout)
    one(grad[1].astype(F32), delta[1].astype(F32), up, mup, gup, nup, nmup)
    one(grad[2].astype(F32), delta[2].astype(F32), down, mdown, gdown, ndown, nmdown)
    n = ga.shape[1]
    for row, (w, m, g_o, w_o, m_o) in enumerate(((ga, ma, gga, nga, nma), (gf, mf, ggf, ngf, nmf))):
        for zz in range(4):
            @pl.when(z == zz)
            def _():
                g_o[...] = gs[row : row + 1, zz * n : zz * n + n]
        new = 0.5 * m[...] + g_o[...]
        m_o[...] = new
        w_o[...] = w[...] - 0.3 * new


def epilogue(grad, delta, gs, bo, ig, w, m):
    vm = pl.BlockSpec(memory_space=pltpu.VMEM)
    sd = lambda a: jax.ShapeDtypeStruct(a.shape, F32)
    ws = tuple(sd(a) for a in w)
    return pl.pallas_call(
        epilogue_kernel,
        out_shape=(jax.ShapeDtypeStruct(bo.shape, BF16), sd(ig)) + ws * 3,
        in_specs=[vm] * 17, out_specs=(vm,) * 20,
        name="epilogue",
    )(grad, delta, gs, bo, ig, *w, *m)


UNITS = ((1, 0, 4, True), (2, 0, 4, False), (0, 0, 2, True), (0, 2, 2, False))
def whole_kernel(scale, shapes, names, *refs):
    r = dict(zip(names, refs))
    rep, z, fr, s, t = place()
    y, x = s // 2, lax.rem(s, 2)
    me = z * 8 + s * 2 + t
    other = {"tp": 1 - t}

    def zdev(k):
        return {"fsdp": lax.rem(z + k, 4) * rep + fr}

    def sidx(j):
        yy, xx = y, x
        if j & 2:
            yy = 1 - y
        if j & 1:
            xx = 1 - x
        return yy * 2 + xx

    def sdev(j):
        return {"seq": sidx(j)}

    def dev(i):
        return {"fsdp": (i // 8) * rep + fr, "seq": lax.rem(i // 2, 4), "tp": lax.rem(i, 2)}

    def al(v, n):
        return pl.multiple_of(v, n)

    def rows(zz, yy=None):
        return pl.ds(al(zz * 96, 32), 96) if yy is None else pl.ds(al(zz * 96 + yy * 48, 16), 48)

    def cols(tt, xx=None):
        return pl.ds(al(tt * 768, 128), 768) if xx is None else pl.ds(al(tt * 768 + xx * 384, 128), 384)

    def r48(yy):
        return pl.ds(al(yy * 48, 16), 48)

    def c384(xx):
        return pl.ds(al(xx * 384, 128), 384)

    bar = pltpu.get_barrier_semaphore()
    near = [zdev(k) for k in range(1, 4)] + [sdev(j) for j in range(1, 4)] + [other]
    near += [{"fsdp": z * rep + lax.rem(fr + b, rep)} for b in range(1, rep)]
    for d in near:
        pl.semaphore_signal(bar, inc=1, device_id=d, device_id_type=MESH)
    wsh, mom, pk = r["wsh"], r["mom"], r["pk"]
    for pre, dst in (("w", wsh), ("m", mom)):
        for i in range(3):
            put_cols(pk, *SPOTS[i], r[pre + "qkv"][i], t)
        put_cols(pk, *SPOTS[3], r[pre + "out"][...].T, t)
        dst[0] = pk[...].astype(dst.dtype)
        dst[1] = r[pre + "up"][...].astype(dst.dtype)
        dst[2] = r[pre + "down"][...].astype(dst.dtype)
    n = 96
    gv = r["gv"]
    gv[...] = jnp.zeros(gv.shape, gv.dtype)
    gv[0:1, 0:n] = r["wga"][...]
    gv[1:2, 0:n] = r["wgf"][...]
    r["gvh"][...] = gv[...].astype(BF16)
    pl.semaphore_wait(bar, len(near))

    sends = []

    def go(c):
        c.start()
        sends.append(c)
        return c

    w = r["w"]
    order = (0, 1, 2)
    zc, pc, pp, own = {}, {}, {}, {}
    locs = []

    def keep(c):
        c.start()
        locs.append(c)
        return c

    for m in order:
        for k in range(1, 4):
            src = wsh.at[m, r48(y), c384(x)]
            zc[m, k] = go(remote(src, w.at[m, rows(z, y), cols(t, x)], r["w_zs"].at[m, k - 1], r["w_zr"].at[m, k - 1], zdev(k)))
        if m == 0:
            gc = [go(remote(r["gvh"], r["gains"].at[z], r["gv_s"].at[k - 1], r["gv_r"].at[k - 1], zdev(k))) for k in range(1, 4)]
    seg = pl.ds(al(s * 64, 64), 64)

    def rows_in(a, src, dst):
        keep(pltpu.make_async_copy(src.at[s, t], dst.at[seg], r["loc"].at[a]))
        return [go(remote(src.at[sidx(j), t], dst.at[seg], r["t_s"].at[a, j - 1], r["t_r"].at[a, j - 1], sdev(j))) for j in range(1, 4)]

    tc = rows_in(0, r["tok"], r["xin"])
    for m in order:
        own[m] = go(remote(wsh.at[m], w.at[m, rows(z), cols(t)], r["w_ps"].at[m, 0], r["w_pr"].at[m, 0], other))
        keep(pltpu.make_async_copy(wsh.at[m], w.at[m, rows(z), cols(t)], r["loc"].at[2 + m]))
    keep(pltpu.make_async_copy(r["gvh"], r["gains"].at[z], r["loc"].at[5]))

    def chunk(m, k, j):
        zk = lax.rem(z + 4 - k, 4)
        sj = sidx(j)
        return w.at[m, rows(zk, sj // 2), cols(t, lax.rem(sj, 2))]

    def plane(m):
        for k in range(1, 4):
            zc[m, k].wait_recv()
            blk = chunk(m, k, 0)
            for j in (1, 2):
                pc[m, k, j] = go(remote(blk, blk, r["w_ls"].at[m, k - 1, j - 1], r["w_lr"].at[m, k - 1, j - 1], sdev(j)))

    def relay(m):
        for k in range(1, 4):
            via = 1 + (m + k) % 2
            pc[m, k, via].wait_recv()
            blk = chunk(m, k, via)
            pc[m, k, 3] = go(remote(blk, blk, r["w_ls"].at[m, k - 1, 2], r["w_lr"].at[m, k - 1, 2], sdev(3 - via)))

    def across(m):
        for k in range(1, 4):
            pc[m, k, 2 - (m + k) % 2].wait_recv()
            pc[m, k, 3].wait_recv()
            blk = w.at[m, rows(lax.rem(z + 4 - k, 4)), cols(t)]
            pp[m, k] = go(remote(blk, blk, r["w_ps"].at[m, k], r["w_pr"].at[m, k], other))

    def landed(m):
        own[m].wait_recv()
        for k in range(1, 4):
            pp[m, k].wait_recv()

    for c in tc + gc:
        c.wait_recv()
    for c in locs:
        c.wait()
    gone = len(locs)
    gfull = r["gfull"]
    for zz in range(4):
        gfull[:, zz * n : zz * n + n] = r["gains"][zz, 0:8, 0:n].astype(F32)
    attn_use, ffn_use = gfull[0:1, :], gfull[1:2, :]
    xin = r["xin"][...].astype(F32)
    plain_attn, inv_attn = stats(xin)
    norm_attn = (plain_attn * attn_use).astype(BF16)
    plane(0)
    cc_ = rows_in(1, r["cot"], r["gin"])
    relay(0)
    natr = r["natr"]
    natr[0] = norm_attn.astype(F32).T.astype(BF16)
    plane(1)
    across(0)
    relay(1)
    landed(0)
    length = r["len"][s, t]
    lanes = lax.broadcasted_iota(jnp.int32, (1, 128), 1)
    low = lanes < 64
    half = 768
    wn, qkv, wts, prb, att, back = (r[name] for name in ("wn", "qkv", "wts", "prb", "att", "back"))
    raw, gsum = r["raw"], r["gsum"]
    for i, (tile, mixed, first) in enumerate(((0, 2, True), (1, 2, False), (3, 5, True), (4, 5, False))):
        wn[i, :, 0:128] = w[0, :, tile * 128 : tile * 128 + 128]
        wn[i, :, 256:384] = w[0, :, half + tile * 128 : half + tile * 128 + 128]
        a = w[0, :, mixed * 128 : mixed * 128 + 128]
        b = w[0, :, half + mixed * 128 : half + mixed * 128 + 128]
        if first:
            wn[i, :, 128:256] = jnp.where(low, a, b)
        else:
            wn[i, :, 128:256] = pltpu.roll(jnp.where(low, b, a).astype(F32), 64, 1).astype(BF16)
    for i in range(3):
        qkv[i] = mm(norm_attn, wn[i]).astype(BF16)
    plane(2)
    nrow = xin.shape[0]
    valid = lax.broadcasted_iota(jnp.int32, (nrow, 1), 0) < length
    hscale = 64 ** (-0.5)
    for p in range(3):
        sl = slice(p * 128, p * 128 + 128)
        q, k, v = qkv[0, :, sl], qkv[1, :, sl], qkv[2, :, sl]
        parts = []
        for h in range(2):
            sel = low if h == 0 else ~low
            sc = mm_nt(k, jnp.where(sel, q, jnp.zeros_like(q))) * hscale
            sc = jnp.where(valid, sc, -jnp.inf)
            e = jnp.exp(sc - jnp.max(sc, axis=0, keepdims=True))
            wt = e * (1.0 / jnp.sum(e, axis=0, keepdims=True))
            wts[2 * p + h] = wt
            pb = wt.astype(BF16)
            prb[2 * p + h] = pb
            parts.append(mm_tn(pb, v))
        att[:, sl] = jnp.where(low, parts[0], parts[1]).astype(BF16)
        if p == 0:
            across(1)
        if p == 1:
            relay(2)
    middle = xin + mm_nt(att[...], wn[3])
    plain_ffn, inv_ffn = stats(middle)
    norm_ffn = (plain_ffn * ffn_use).astype(BF16)
    natr[1] = norm_ffn.astype(F32).T.astype(BF16)
    for c in cc_:
        c.wait_recv()
    locs[gone].wait()
    upstream = r["gin"][...]
    natr[2] = upstream.astype(F32).T.astype(BF16)
    across(2)
    landed(1)
    landed(2)

    prx = r["prx"]
    pair = {}

    def send_pair(m):
        pair[m] = go(remote(raw.at[m, :, cols(1 - t)], prx.at[m], r["p_s"].at[m], r["p_r"].at[m], other))

    first, second = {}, {}

    def stage_first(u):
        m, f0, nf, xfirst = UNITS[u]
        rr = slice(f0 * 96, f0 * 96 + nf * 96)
        fs, fo = r["fs%d" % u], r["fo%d" % u]
        if xfirst:
            fs[...] = (raw[m, rr, cols(t, 1 - x)].astype(F32) + prx[m, rr, c384(1 - x)].astype(F32)).astype(BF16)
            fo[...] = raw[m, rr, cols(t, x)].astype(F32) + prx[m, rr, c384(x)].astype(F32)
        else:
            for f in range(nf):
                far = pl.ds(al((f0 + f) * 96 + (1 - y) * 48, 16), 48)
                near = pl.ds(al((f0 + f) * 96 + y * 48, 16), 48)
                fs[f] = (raw[m, far, cols(t)].astype(F32) + prx[m, far, :].astype(F32)).astype(BF16)
                fo[f] = raw[m, near, cols(t)].astype(F32) + prx[m, near, :].astype(F32)
        first[u] = go(remote(fs, r["fr%d" % u], r["f_s"].at[u], r["f_r"].at[u], sdev(1 if xfirst else 2)))

    part = r["part"]

    def stage_second(u):
        m, f0, nf, xfirst = UNITS[u]
        first[u].wait_recv()
        fo, fr_, ss = r["fo%d" % u], r["fr%d" % u], r["ss%d" % u]
        for f in range(nf):
            if xfirst:
                far = pl.ds(al(f * 96 + (1 - y) * 48, 16), 48)
                near = pl.ds(al(f * 96 + y * 48, 16), 48)
                ss[f] = (fo[far, :] + fr_[far, :].astype(F32)).astype(BF16)
                part[m, f0 + f] = fo[near, :] + fr_[near, :].astype(F32)
            else:
                ss[f] = (fo[f, :, c384(1 - x)] + fr_[f, :, c384(1 - x)].astype(F32)).astype(BF16)
                part[m, f0 + f] = fo[f, :, c384(x)] + fr_[f, :, c384(x)].astype(F32)
        second[u] = go(remote(ss, r["sr%d" % u], r["s_s"].at[u], r["s_r"].at[u], sdev(2 if xfirst else 1)))

    gz = {}

    def stage_z(m):
        for u, (mu, f0, nf, xfirst) in enumerate(UNITS):
            if mu == m:
                second[u].wait_recv()
                for f in range(nf):
                    part[m, f0 + f] = part[m, f0 + f] + r["sr%d" % u][f].astype(F32)
        for k in range(1, 4):
            r["zs"][m, k - 1] = part[m, lax.rem(z + k, 4)].astype(BF16)
            gz[m, k] = go(remote(r["zs"].at[m, k - 1], r["zr"].at[m, k - 1], r["z_s"].at[m, k - 1], r["z_r"].at[m, k - 1], zdev(k)))

    fins = []
    mbuf, mb, da = r["mbuf"], r["mb"], r["da"]

    def piece(src, dst, so, to, i):
        for k in range(4):
            dev_k = {"fsdp": lax.rem(z + k, 4) * rep + fr, "seq": so, "tp": to}
            c = remote(src, dst, r["o_s"].at[i, k], r["m_r"].at[me], dev_k)
            if k:
                c.start()
                fins.append(c.wait_send)
            else:
                mine = (s == so) & (t == to)

                @pl.when(~mine)
                def _():
                    c.start()

                @pl.when(mine)
                def _():
                    pltpu.make_async_copy(src, dst, r["m_r"].at[me]).start()

                def fin(mine=mine, c=c):
                    @pl.when(~mine)
                    def _():
                        c.wait_send()

                fins.append(fin)

    ac = []
    grad_sh, delta_sh, mom = r["grad_sh"], r["delta_sh"], r["mom"]

    def stage_final(m):
        tot = part[m, z]
        for k in range(1, 4):
            gz[m, k].wait_recv()
            tot = tot + r["zr"][m, k - 1].astype(F32)
        if rep > 1:
            r["rs"][m] = tot.astype(BF16)
            rc = [go(remote(r["rs"].at[m], r["rr"].at[m, b - 1], r["r_s"].at[m, b - 1], r["r_r"].at[m, b - 1], {"fsdp": z * rep + lax.rem(fr + b, rep)})) for b in range(1, rep)]
            for b in range(1, rep):
                rc[b - 1].wait_recv()
                tot = tot + r["rr"][m, b - 1].astype(F32)
        half_g = (tot * scale).astype(BF16)
        grad_sh[m, r48(y), c384(x)] = half_g
        new = (0.5 * mom[m, r48(y), c384(x)] + half_g.astype(F32)).astype(BF16)
        if m:
            mb[m - 1] = new
            for b in range(2):
                piece(mb.at[m - 1], mbuf.at[rows(z, y), cols(t, x)], 2 * (m - 1) + b, 1, 2 * (m - 1) + b)
        else:
            for b in range(2):
                r["ma"][b, :, 0:128] = new[:, b * 128 : b * 128 + 128]
                r["ma"][b, :, 128:256] = new[:, 256:384]
                piece(r["ma"].at[b], mbuf.at[rows(z, y), pl.ds(al(t * 256, 128), 256)], 2 * b + x, 0, 4 + b)
        blk = grad_sh.at[m, r48(y), c384(x)]
        for j in range(1, 4):
            ac.append(go(remote(blk, blk, r["a_s"].at[m, j - 1], r["a_r"].at[m, j - 1], sdev(j))))

    def images(a, src, dst):
        for j in range(4):
            blk = src.at[pl.ds(al(sidx(j) * 64, 64), 64)]
            if j:
                ic.append(go(remote(blk, dst.at[s, t], r["i_s"].at[a, j - 1], r["i_r"].at[a, j - 1], sdev(j))))
            else:
                keep(pltpu.make_async_copy(blk, dst.at[s, t], r["loc"].at[6 + a]))

    ic = []

    acc_out = jnp.zeros(xin.shape, F32)
    acc_back = jnp.zeros(xin.shape, F32)
    width = 256
    for c in range(1536 // width):
        cs = pl.ds(al(lax.rem(768 * (1 - t) + c * width, 1536), width), width)
        up, down = w[1, :, cs], w[2, :, cs]
        hidden = mm(norm_ffn, up)
        cdf = 0.5 * (1.0 + lax.erf(hidden * 0.7071067811865476))
        act = (hidden * cdf).astype(BF16)
        back_act = mm(upstream, down)
        pdf = 0.3989422804014327 * jnp.exp(-0.5 * hidden * hidden)
        bh = (back_act * (cdf + hidden * pdf)).astype(BF16)
        acc_out = acc_out + mm_nt(act, down)
        acc_back = acc_back + mm_nt(bh, up)
        raw[1, :, cs] = mm(natr[1], bh).astype(BF16)
        raw[2, :, cs] = mm(natr[2], act).astype(BF16)
        if 2 * (c + 1) * width == 1536:
            send_pair(1)
            send_pair(2)
    pair[1].wait_recv()
    stage_first(0)
    pair[2].wait_recv()
    stage_first(1)
    r["bo"][...] = (middle + acc_out).astype(BF16)
    gsum[...] = jnp.zeros_like(gsum)
    gsum[1:2, :] = jnp.sum(acc_back * plain_ffn, axis=0, keepdims=True)
    back_middle = upstream.astype(F32) + norm_back(acc_back, plain_ffn, inv_ffn, ffn_use)
    mh = back_middle.astype(BF16)
    ba = mm(mh, wn[3]).astype(BF16)

    raw_n = r["raw_n"]
    for p in range(3):
        sl = slice(p * 128, p * 128 + 128)
        q, k, v = qkv[0, :, sl], qkv[1, :, sl], qkv[2, :, sl]
        bap = ba[:, sl]
        bq, bk, bv = [], [], []
        for h in range(2):
            sel = low if h == 0 else ~low
            bp = mm_nt(v, jnp.where(sel, bap, jnp.zeros_like(bap)))
            wt = wts[2 * p + h]
            dl = jnp.sum(wt * bp, axis=0, keepdims=True)
            ds = (wt * (bp - dl) * hscale).astype(BF16)
            bq.append(mm_tn(ds, k))
            bk.append(mm(ds, q))
            bv.append(mm(prb[2 * p + h], bap))
        back[0, :, sl] = jnp.where(low, bq[0], bq[1]).astype(BF16)
        back[1, :, sl] = jnp.where(low, bk[0], bk[1]).astype(BF16)
        back[2, :, sl] = jnp.where(low, bv[0], bv[1]).astype(BF16)
    for i in range(3):
        raw_n[i] = mm(natr[0], back[i])
    raw_n[3] = mm(mh.astype(F32).T.astype(BF16), att[...])
    for a, b, tile, mixed in ((0, 1, 0, 2), (2, 3, 3, 5)):
        for i, tl in ((a, tile), (b, tile + 1)):
            raw[0, :, tl * 128 : tl * 128 + 128] = raw_n[i, :, 0:128].astype(BF16)
            raw[0, :, half + tl * 128 : half + tl * 128 + 128] = raw_n[i, :, 256:384].astype(BF16)
        lead = raw_n[a, :, 128:256]
        tail = pltpu.roll(raw_n[b, :, 128:256], 64, 1)
        raw[0, :, mixed * 128 : mixed * 128 + 128] = jnp.where(low, lead, tail).astype(BF16)
        raw[0, :, half + mixed * 128 : half + mixed * 128 + 128] = jnp.where(low, tail, lead).astype(BF16)
    send_pair(0)
    stage_second(0)
    back_attn = jnp.zeros(xin.shape, F32)
    for i in range(3):
        back_attn = back_attn + mm_nt(back[i], wn[i])
    gsum[0:1, :] = jnp.sum(back_attn * plain_attn, axis=0, keepdims=True)
    gc = go(remote(gsum, r["g1"], r["g_s"].at[0], r["g_r"].at[0], other))
    pair[0].wait_recv()
    stage_first(2)
    stage_first(3)
    stage_second(1)
    r["ig"][...] = (back_middle + norm_back(back_attn, plain_attn, inv_attn, attn_use)).astype(BF16)
    gst, gzz = r["gst"], r["gzz"]
    gc.wait_recv()
    gst[0] = gsum[...] + r["g1"][...]
    gc = go(remote(gst.at[0], r["g2"], r["g_s"].at[1], r["g_r"].at[1], sdev(1)))
    stage_z(1)
    stage_second(2)
    stage_second(3)
    stage_z(2)
    gc.wait_recv()
    gst[1] = gst[0] + r["g2"][...]
    gc = go(remote(gst.at[1], r["g3"], r["g_s"].at[2], r["g_r"].at[2], sdev(2)))
    stage_final(1)
    stage_z(0)
    stage_final(2)
    stage_final(0)
    gc.wait_recv()
    gzz[pl.ds(z, 1)] = (gst[1] + r["g3"][...])[None]
    gcs = [go(remote(gzz.at[z], gzz.at[z], r["g_s"].at[2 + k], r["g_r"].at[2 + k], zdev(k))) for k in range(1, 4)]
    for c in gcs:
        c.wait_recv()
    gtot = (gzz[0] + gzz[1]) + (gzz[2] + gzz[3])
    if rep > 1:
        r["grs"][pl.ds(fr, 1)] = gtot[None]
        grc = [go(remote(r["grs"].at[fr], r["grs"].at[fr], r["gr_s"].at[b - 1], r["gr_r"].at[b - 1], {"fsdp": z * rep + lax.rem(fr + b, rep)})) for b in range(1, rep)]
        for c in grc:
            c.wait_recv()
        gtot = r["grs"][0]
        for b in range(1, rep):
            gtot = gtot + r["grs"][b]
    r["gs_out"][...] = gtot * scale
    images(0, r["bo"], r["bo_out"])
    images(1, r["ig"], r["ig_out"])

    def arrivals():
        @pl.when(t == 1)
        def _():
            def arrive(i, carry):
                pltpu.make_async_copy(mb.at[0], mbuf.at[pl.ds(0, 48), pl.ds(0, 384)], r["m_r"].at[i]).wait()
                return carry

            lax.fori_loop(0, 32, arrive, 0)

        @pl.when(t == 0)
        def _():
            def arrive(i, carry):
                j = (i // 4) * 8 + (lax.rem(i, 4) // 2) * 4 + x * 2 + lax.rem(i, 2)
                pltpu.make_async_copy(r["ma"].at[0], mbuf.at[pl.ds(0, 48), pl.ds(0, 256)], r["m_r"].at[j]).wait()
                return carry

            lax.fori_loop(0, 16, arrive, 0)

    arrivals()
    dw = r["dw"]
    newton_schulz(z, s, t, mbuf, da, dw, r["gram"])

    delta_sh = r["delta_sh"]
    outgoing = []
    for j in range(4):
        @pl.when(t == 0)
        def _():
            for tt in range(2):
                src, dst = da.at[tt], r["din"].at[s]
                if j:
                    remote(src, dst, r["d_s"].at[j, tt], r["d_r"].at[s], {"seq": sidx(j), "tp": tt}).start()
                elif tt:
                    remote(src, dst, r["d_s"].at[j, tt], r["d_r"].at[s], {"tp": tt}).start()
                else:
                    pltpu.make_async_copy(src, dst, r["d_r"].at[s]).start()

        @pl.when(t == 1)
        def _():
            m, tt = 1 + s // 2, lax.rem(s, 2)
            dst = delta_sh.at[m]
            if j:
                remote(dw, dst, r["d_s"].at[j, 0], r["d_r"].at[3 + m], {"seq": sidx(j), "tp": tt}).start()
            else:
                @pl.when(tt == 0)
                def _():
                    remote(dw, dst, r["d_s"].at[j, 0], r["d_r"].at[3 + m], {"tp": 0}).start()

                @pl.when(tt == 1)
                def _():
                    pltpu.make_async_copy(dw, dst, r["d_r"].at[3 + m]).start()

    for c in ic:
        c.wait_recv()
    for c in locs[gone + 1 :]:
        c.wait()
    oc = [go(remote(dst.at[:, t], dst.at[:, t], r["i_s"].at[a, 3], r["i_r"].at[a, 3], other)) for a, dst in enumerate((r["bo_out"], r["ig_out"]))]
    for c in ac:
        c.wait_recv()
    din = r["din"]
    for i in range(4):
        pltpu.make_async_copy(da.at[0], din.at[i], r["d_r"].at[i]).wait()
    for i in range(2):
        delta_sh[0, :, i * 384 : i * 384 + 128] = din[i, :, 0:128]
        delta_sh[0, :, i * 384 + 128 : i * 384 + 256] = din[2 + i, :, 0:128]
        lead = jnp.where(low, 0, 1) == t
        delta_sh[0, :, i * 384 + 256 : i * 384 + 384] = jnp.where(lead, din[i, :, 128:256], din[2 + i, :, 128:256])
    for m in (1, 2):
        pltpu.make_async_copy(dw, delta_sh.at[m], r["d_r"].at[3 + m]).wait()
    for c in oc:
        c.wait_recv()
    for c in sends:
        c.wait_send()
    for f in fins:
        f()
    for j in range(4):
        @pl.when(t == 0)
        def _():
            for tt in range(2):
                if j or tt:
                    remote(da.at[tt], din.at[s], r["d_s"].at[j, tt], r["d_r"].at[s], {"seq": sidx(j), "tp": tt}).wait_send()

        @pl.when(t == 1)
        def _():
            m, tt = 1 + s // 2, lax.rem(s, 2)
            c = remote(dw, delta_sh.at[m], r["d_s"].at[j, 0], r["d_r"].at[3 + m], {"seq": sidx(j), "tp": tt})
            if j:
                c.wait_send()
            else:
                @pl.when(tt == 0)
                def _():
                    c.wait_send()


def whole(scale, rep, lengths, tok, cot, weights, moments):
    vm = pl.BlockSpec(memory_space=pltpu.VMEM)
    anyw = pl.BlockSpec(memory_space=pl.ANY)
    D = pltpu.SemaphoreType.DMA
    V = pltpu.VMEM
    d = tok.shape[-1]
    seg = tok.shape[2]
    n = 4 * seg
    parts = ("qkv", "out", "up", "down", "ga", "gf")
    ins = ["len", "tok", "cot"] + ["w" + p for p in parts] + ["m" + p for p in parts[:4]]
    outs = {
        "grad_sh": ((3, 96, 768), BF16), "delta_sh": ((3, 96, 768), BF16),
        "bo_out": ((4, 2, seg, d), BF16), "ig_out": ((4, 2, seg, d), BF16), "gs_out": ((8, d), F32),
    }
    scr = {
        "wsh": V((3, 96, 768), BF16), "mom": V((3, 96, 768), F32), "pk": V((96, 768), F32), "gv": V((16, 128), F32), "gvh": V((16, 128), BF16),
        "w": V((3, d, 4 * d), BF16), "gains": V((4, 16, 128), BF16), "gfull": V((8, d), F32),
        "xin": V((n, d), BF16), "gin": V((n, d), BF16),
        "wn": V((4, d, d), BF16), "qkv": V((3, n, d), BF16), "wts": V((6, n, n), F32), "prb": V((6, n, n), BF16),
        "att": V((n, d), BF16), "back": V((3, n, d), BF16), "natr": V((3, d, n), BF16), "raw_n": V((4, d, d), F32),
        "raw": V((3, d, 4 * d), BF16), "gsum": V((8, d), F32), "bo": V((n, d), BF16), "ig": V((n, d), BF16),
        "prx": V((3, d, 768), BF16), "part": V((3, 4, 48, 384), F32),
        "zs": V((3, 3, 48, 384), BF16), "zr": V((3, 3, 48, 384), BF16), "mb": V((2, 48, 384), BF16), "ma": V((2, 48, 256), BF16),
        "mbuf": V((384, 1536), BF16), "da": V((2, 96, 256), BF16), "din": V((4, 96, 256), BF16), "dw": V((96, 768), BF16),
        "gram": V((384, 384), F32),
        "g1": V((8, d), F32), "g2": V((8, d), F32), "g3": V((8, d), F32), "gzz": V((4, 8, d), F32), "gst": V((2, 8, d), F32),
        "w_zs": D((3, 3)), "w_zr": D((3, 3)), "w_ls": D((3, 3, 3)), "w_lr": D((3, 3, 3)), "w_ps": D((3, 4)), "w_pr": D((3, 4)),
        "gv_s": D((3,)), "gv_r": D((3,)), "t_s": D((2, 3)), "t_r": D((2, 3)), "loc": D((8,)),
        "p_s": D((3,)), "p_r": D((3,)), "f_s": D((4,)), "f_r": D((4,)), "s_s": D((4,)), "s_r": D((4,)),
        "z_s": D((3, 3)), "z_r": D((3, 3)), "a_s": D((3, 3)), "a_r": D((3, 3)), "o_s": D((6, 4)), "m_r": D((32,)),
        "d_s": D((4, 2)), "d_r": D((6,)), "i_s": D((2, 4)), "i_r": D((2, 4)),
        "g_s": D((6,)), "g_r": D((6,)),
    }
    for u, (m, f0, nf, xfirst) in enumerate(UNITS):
        a = (nf * 96, 384) if xfirst else (nf, 48, 768)
        scr["fs%d" % u] = V(a, BF16)
        scr["fr%d" % u] = V(a, BF16)
        scr["fo%d" % u] = V(a, F32)
        scr["ss%d" % u] = V((nf, 48, 384), BF16)
        scr["sr%d" % u] = V((nf, 48, 384), BF16)
    if rep > 1:
        scr.update({"rs": V((3, 48, 384), BF16), "rr": V((3, rep - 1, 48, 384), BF16), "r_s": D((3, rep - 1)), "r_r": D((3, rep - 1)),
                    "grs": V((rep, 8, d), F32), "gr_s": D((rep - 1,)), "gr_r": D((rep - 1,))})
    names = ins + list(outs) + list(scr)
    return pl.pallas_call(
        functools.partial(whole_kernel, scale, None, names),
        out_shape=tuple(jax.ShapeDtypeStruct(*o) for o in outs.values()),
        in_specs=[pl.BlockSpec(memory_space=pltpu.SMEM), anyw, anyw] + [vm] * 10, out_specs=(vm,) * 5,
        scratch_shapes=list(scr.values()),
        compiler_params=pltpu.CompilerParams(collective_id=0, has_side_effects=True, vmem_limit_bytes=60 * 1024 * 1024),
        name="whole",
    )(lengths, tok, cot, *weights, *moments)


def body(tokens, lengths, grad_out, *params):
    micro, img_dev, tok_loc, width = tokens.shape
    fsdp = lax.axis_size("fsdp")
    rep = fsdp // 4
    fi = lax.axis_index("fsdp")
    scale = (micro * img_dev * fsdp * tok_loc * lax.axis_size("seq")) ** (-0.5)
    groups = [[a * rep + b for b in range(rep)] for a in range(4)]
    split_dims = (1, 1, 0, 1, 0, 0)

    def ready(values):
        if rep > 1:
            values = [lax.all_gather(a, "fsdp", axis=d, tiled=True, axis_index_groups=groups) for a, d in zip(values, split_dims)]
        qkv, out, up, down, ga, gf = values
        return [qkv, out, up, down.T, ga[None], gf[None]]

    def done(values):
        qkv, out, up, down, ga, gf = values
        values = [qkv, out, up, down.T, ga[0], gf[0]]
        if rep > 1:
            fr = lax.rem(fi, rep)
            values = [lax.dynamic_slice_in_dim(a, fr * (a.shape[d] // rep), a.shape[d] // rep, axis=d) for a, d in zip(values, split_dims)]
        return values

    w, m = ready(params[:6]), ready(params[6:])
    grad, delta, bo, ig, gs = whole(scale, rep, lengths, tokens, grad_out, w, m[:4])
    o = epilogue(grad, delta, gs, bo, ig, w, m)
    return tuple(o[:2]) + tuple(done(o[2:8])) + tuple(done(o[8:14])) + tuple(done(o[14:]))


def solution(mesh):
    weights = (P(None, "fsdp", "tp"), P("tp", "fsdp"), P("fsdp", "tp"), P("tp", "fsdp"), P("fsdp"), P("fsdp"))
    rows = P(None, "fsdp", "seq", None)
    return jax.shard_map(body, mesh=mesh, in_specs=(rows, P(None, "fsdp"), rows) + weights + weights,
                         out_specs=(rows, rows) + weights + weights + weights, check_vma=False)
```
